32 devices in a mesh: row: 4 (over z), col: 2 (over x), depth: 4 (over y, core).
Axes of the slice: x: 2, y: 2, z: 4, core: 2. Of those that a mesh axis runs over, the one named last changes fastest.
Arguments:
- pair_input: bfloat16 [192, 192, 128], P('row', ('col', 'depth')), may hold values from -40 to 40
- in_gain: float32 [128], replicated, may hold values from 0.1 to 1.9
- in_shift: float32 [128], replicated, may hold values from -3 to 3
- w_proj: bfloat16 [128, 512], replicated, may hold values from -0.5 to 0.5
- w_gate: bfloat16 [128, 128], replicated, may hold values from -0.5 to 0.5
- out_gain: float32 [128], replicated, may hold values from 0.1 to 1.9
- out_shift: float32 [128], replicated, may hold values from -3 to 3
- w_out: bfloat16 [128, 128], replicated, may hold values from -0.5 to 0.5
Outputs:
- update: bfloat16 [192, 192, 128], P('row', ('col', 'depth'))
The draws below stay inside these ranges and needn't reach their ends.
All inputs are finite; a program needn't handle non-finite values.
Results may differ from the reference program's by a relative error of at most 0.013.
Values may be sent and summed in bfloat16 or wider, within the bound.
No kernel may reach another device: no remote copies, remote signals or barrier semaphores. Data moves between devices by JAX's collectives and lax.ppermute only.
A program may use at most 64 MiB of HBM per device.

```python
import math
import jax
import jax.numpy as jnp
from jax import lax

C_Z = 128
C = 128
RESIDUES = 192


def draw_pair_input(key, part):
    key_entries = jax.random.fold_in(key, 11)
    key_scales = jax.random.fold_in(key, 12)
    scales = jnp.exp(jax.random.uniform(key_scales, (RESIDUES, RESIDUES, 1), jnp.float32, 0.0, math.log(10.0)))
    entries = jnp.clip(jax.random.normal(key_entries, (RESIDUES, RESIDUES, C_Z), jnp.float32), -4.0, 4.0)
    values = entries * scales
    return values.astype(jnp.bfloat16)


def gaussian(stream_key, shape, width, most, kind=jnp.bfloat16):
    return jnp.clip(width * jax.random.normal(stream_key, shape, jnp.float32), -most, most).astype(kind)


def setup_inputs(seed: int = 0) -> dict:
    splits = jax.random.split(jax.random.key(seed), 9)
    return {
        "pair_input": draw_pair_input(jax.random.fold_in(splits[8], 71), 0),
        "in_gain": jnp.clip(1.0 + 0.18 * jax.random.normal(splits[1], (C_Z,), jnp.float32), 0.1, 1.9),
        "in_shift": gaussian(splits[2], (C_Z,), 0.5, 3.0, jnp.float32),
        "w_proj": gaussian(splits[3], (C_Z, 4 * C), C_Z ** -0.5, 0.5),
        "w_gate": gaussian(splits[4], (C_Z, C_Z), C_Z ** -0.5, 0.5),
        "out_gain": jnp.clip(1.0 + 0.18 * jax.random.normal(splits[5], (C,), jnp.float32), 0.1, 1.9),
        "out_shift": gaussian(splits[6], (C,), 0.5, 3.0, jnp.float32),
        "w_out": gaussian(splits[7], (C, C_Z), C ** -0.5, 0.5),
    }


def layer_norm(values, scaling, offsets):
    average = lax.optimization_barrier(jnp.mean(values, axis=-1, keepdims=True))
    centred = values - average
    variance = lax.optimization_barrier(jnp.mean(centred * centred, axis=-1, keepdims=True))
    return centred * lax.rsqrt(variance + 1e-05) * scaling + offsets

def reference(pair_input, in_gain, in_shift, w_proj, w_gate, out_gain, out_shift, w_out):
    normed = layer_norm(pair_input.astype(jnp.float32), in_gain, in_shift).astype(jnp.bfloat16)
    channels = w_proj.shape[1] // 4

    def side_rows(normed_row):
        projected = jnp.dot(normed_row, w_proj, preferred_element_type=jnp.float32)
        left_side = (jax.nn.sigmoid(projected[:, :channels]) * projected[:, channels:2 * channels]).astype(jnp.bfloat16)
        right_side = (jax.nn.sigmoid(projected[:, 2 * channels:3 * channels]) * projected[:, 3 * channels:]).astype(jnp.bfloat16)
        return (left_side, right_side)
    left_side, right_side = lax.map(side_rows, normed)
    product = jnp.einsum('kic,kjc->ijc', left_side.astype(jnp.float32), right_side.astype(jnp.float32), precision=lax.Precision.HIGHEST)
    product_norm = layer_norm(product, out_gain, out_shift).astype(jnp.bfloat16)
    gating = jax.nn.sigmoid(jnp.einsum('xyc,cd->xyd', normed.astype(jnp.float32), w_gate.astype(jnp.float32), precision=lax.Precision.HIGHEST))
    projected_out = jnp.einsum('xyc,cd->xyd', product_norm.astype(jnp.float32), w_out.astype(jnp.float32), precision=lax.Precision.HIGHEST)
    return (gating * projected_out).astype(jnp.bfloat16)
```

```python
import functools

import jax
import jax.numpy as jnp
from jax import lax
from jax.experimental import pallas as pl
from jax.experimental.pallas import tpu as pltpu
from jax.sharding import Mesh
from jax.sharding import PartitionSpec as P

LANES = 128
ROWS = 8
NT = (((1,), (1,)), ((), ()))


def layer_norm(values, scaling, offsets):
    average = jnp.mean(values, axis=-1, keepdims=True)
    centred = values - average
    variance = jnp.mean(centred * centred, axis=-1, keepdims=True)
    return centred * lax.rsqrt(variance + 1e-05) * scaling + offsets


def reorder_channels(values, row_count, other_count):
    shape_rest = values.shape[1:]
    grouped = values.reshape((row_count, other_count, -1) + shape_rest)
    return jnp.swapaxes(grouped, 0, 1).reshape(values.shape)


def plain_device(pair_input, in_gain, in_shift, w_proj, w_gate, out_gain, out_shift, w_out):
    row_count = lax.axis_size("row")
    others = ("col", "depth")
    other_count = lax.axis_size("col") * lax.axis_size("depth")
    channels = w_proj.shape[1] // 4
    normed = layer_norm(pair_input.astype(jnp.float32), in_gain, in_shift).astype(jnp.bfloat16)
    projected = jnp.einsum("xyc,cd->xyd", normed, w_proj, preferred_element_type=jnp.float32)
    sides = []
    for at in (0, 2 * channels):
        gate = jax.nn.sigmoid(projected[..., at : at + channels])
        side = (gate * projected[..., at + channels : at + 2 * channels]).astype(jnp.bfloat16)
        side = lax.all_to_all(side, "row", split_axis=2, concat_axis=0, tiled=True)
        sides.append(lax.all_to_all(side, others, split_axis=2, concat_axis=1, tiled=True))
    planes = jnp.einsum("kic,kjc->ijc", *sides, preferred_element_type=jnp.float32)
    product = lax.all_to_all(
        planes.astype(jnp.bfloat16), "row", split_axis=0, concat_axis=2, tiled=True
    )
    product = lax.all_to_all(product, others, split_axis=1, concat_axis=2, tiled=True)
    used = [reorder_channels(a, row_count, other_count) for a in (out_gain, out_shift, w_out)]
    product_norm = layer_norm(product.astype(jnp.float32), used[0], used[1]).astype(jnp.bfloat16)
    gating = jax.nn.sigmoid(
        jnp.einsum("xyc,cd->xyd", normed, w_gate, preferred_element_type=jnp.float32)
    )
    out = jnp.einsum("xyc,cd->xyd", product_norm, used[2], preferred_element_type=jnp.float32)
    return (gating * out).astype(jnp.bfloat16)


def swap_with_lanes(tiles):
    tiles = list(tiles)
    count = len(tiles)
    lane = lax.broadcasted_iota(jnp.int32, tiles[0].shape, 1)
    step = 1
    while step < count:
        upper = (lane & step) != 0
        new = list(tiles)
        for v in range(count):
            if not v & step:
                low, high = tiles[v], tiles[v | step]
                new[v] = jnp.where(upper, pltpu.roll(high, step, 1), low)
                new[v | step] = jnp.where(upper, high, pltpu.roll(low, LANES - step, 1))
        tiles = new
        step *= 2
    return tiles


def side_of(normed, weights, channels):
    projected = jnp.dot(normed, weights, preferred_element_type=jnp.float32)
    return jax.nn.sigmoid(projected[:, :channels]) * projected[:, channels:]


def store_side(side, out_ref, split, k_group, i_tile):
    tiles = [side[s * ROWS : (s + 1) * ROWS] for s in range(split)]
    tiles = swap_with_lanes(tiles)
    for s in range(split):
        out_ref[
            s,
            i_tile * ROWS : (i_tile + 1) * ROWS,
            k_group * LANES : (k_group + 1) * LANES,
        ] = tiles[s].astype(out_ref.dtype)


def left_kernel(split, x_ref, gain_ref, shift_ref, w_ref, normed_ref, out_ref):
    rows, columns, channels = x_ref.shape
    for k_group in range(rows // split):
        for i_tile in range(columns // ROWS):
            at = (slice(k_group * split, (k_group + 1) * split), slice(i_tile * ROWS, (i_tile + 1) * ROWS))
            values = x_ref[at].astype(jnp.float32).reshape(split * ROWS, channels)
            normed = layer_norm(values, gain_ref[...], shift_ref[...])
            normed_ref[at] = normed.reshape(split, ROWS, channels).astype(jnp.bfloat16)
            side = side_of(normed.astype(jnp.bfloat16), w_ref[:, : 2 * channels], channels)
            store_side(side, out_ref, split, k_group, i_tile)


def right_kernel(split, normed_ref, w_ref, out_ref):
    rows, columns, channels = normed_ref.shape
    for k_group in range(rows // split):
        for i_tile in range(columns // ROWS):
            at = (slice(k_group * split, (k_group + 1) * split), slice(i_tile * ROWS, (i_tile + 1) * ROWS))
            normed = normed_ref[at].reshape(split * ROWS, channels)
            side = side_of(normed, w_ref[:, 2 * channels :], channels)
            store_side(side, out_ref, split, k_group, i_tile)


def gate_kernel(normed_ref, w_ref, out_ref):
    rows, columns, channels = normed_ref.shape
    normed = normed_ref[...].reshape(rows * columns, channels)
    gate = jax.nn.sigmoid(jnp.dot(normed, w_ref[...], preferred_element_type=jnp.float32))
    out_ref[...] = gate.reshape(rows, columns, channels)


def product_kernel(split, own_ref, other_ref, right_ref, out_ref):
    row_count, rows, width = own_ref.shape
    columns = rows // row_count
    groups = LANES // split
    right = jnp.concatenate([right_ref[r] for r in range(row_count)], axis=1)
    lane = lax.broadcasted_iota(jnp.int32, (split, row_count * width), 1)
    group = lax.rem(lane, LANES) // split
    for target in range(row_count):
        at = slice(target * columns, (target + 1) * columns)
        left = jnp.concatenate(
            [
                jnp.concatenate([ref[r, at, :] for r in range(row_count)], axis=1)
                for ref in (own_ref, other_ref)
            ],
            axis=0,
        )
        parts = []
        for slab in range(2 * columns // split):
            piece = left[slab * split : (slab + 1) * split]
            for g in range(groups):
                parts.append(jnp.where(group == g, piece, jnp.zeros_like(piece)))
        masked = jnp.concatenate(parts, axis=0)
        block = lax.dot_general(right, masked, NT, preferred_element_type=jnp.float32)
        out_ref[target] = block.astype(out_ref.dtype)


def output_kernel(split, place_ref, sums_ref, gate_ref, gain_ref, shift_ref, w_ref, out_ref):
    _, columns, width = sums_ref.shape
    rows, _, channels = out_ref.shape
    parity = place_ref[0]
    pieces = split // ROWS
    for j_tile in range(columns // ROWS):
        js = slice(j_tile * ROWS, (j_tile + 1) * ROWS)
        for slab in range(width // LANES):
            lanes = slice(slab * LANES, (slab + 1) * LANES)
            tiles = [sums_ref[s, js, lanes].astype(jnp.float32) for s in range(split)]
            tiles = swap_with_lanes(tiles)
            values = jnp.concatenate(tiles, axis=0)
            normed = layer_norm(values, gain_ref[...], shift_ref[...]).astype(jnp.bfloat16)
            projected = jnp.dot(normed, w_ref[...], preferred_element_type=jnp.float32)
            for piece in range(pieces):
                first = slab * split + piece * ROWS
                half, rest = divmod(first, rows // 2)
                block, inside = divmod(rest, columns)
                core = parity if half == 0 else 1 - parity
                at = pl.ds((2 * block + core) * columns + inside, ROWS)
                value = projected[piece * ROWS * ROWS : (piece + 1) * ROWS * ROWS]
                value = value.reshape(ROWS, ROWS, channels)
                out_ref[at, js, :] = (gate_ref[at, js, :] * value).astype(out_ref.dtype)


def call(kernel, name, out_shape, flops, *arrays, scalars=0):
    specs = [pl.BlockSpec(memory_space=pltpu.SMEM)] * scalars
    specs += [pl.BlockSpec(memory_space=pltpu.VMEM)] * (len(arrays) - scalars)
    outs = jax.tree.leaves(out_shape)
    moved = sum(a.size * a.dtype.itemsize for a in [*arrays, *outs])
    return pl.pallas_call(
        kernel,
        name=name,
        out_shape=out_shape,
        in_specs=specs,
        out_specs=jax.tree.map(lambda _: pl.BlockSpec(memory_space=pltpu.VMEM), out_shape),
        cost_estimate=pl.CostEstimate(flops=flops, bytes_accessed=moved, transcendentals=0),
    )(*arrays)


def fast_device(pair_input, in_gain, in_shift, w_proj, w_gate, out_gain, out_shift, w_out):
    rows, columns, channels = pair_input.shape
    row_count = lax.axis_size("row")
    owners = ("row", "col", "depth")
    split = row_count * lax.axis_size("col") * lax.axis_size("depth")
    width = rows // split * LANES
    per_row = split // row_count
    bf16 = jnp.bfloat16
    gains = [a.reshape(1, channels) for a in (in_gain, in_shift, out_gain, out_shift)]
    message = jax.ShapeDtypeStruct((split, columns, width), bf16)
    flops = 4 * rows * columns * channels * channels

    normed, left = call(
        functools.partial(left_kernel, split),
        "left",
        (jax.ShapeDtypeStruct(pair_input.shape, bf16), message),
        flops,
        pair_input,
        gains[0],
        gains[1],
        w_proj,
    )
    exchange = functools.partial(
        lax.all_to_all, axis_name=owners, split_axis=0, concat_axis=0, tiled=True
    )
    own = exchange(left)
    right = exchange(call(functools.partial(right_kernel, split), "right", message, flops, normed, w_proj))
    gate = call(gate_kernel, "gate", jax.ShapeDtypeStruct(pair_input.shape, jnp.float32), flops // 2, normed, w_gate)
    other = lax.ppermute(own, "core", [(0, 1), (1, 0)])
    stacked = (row_count, per_row * columns, width)
    sums = call(
        functools.partial(product_kernel, split),
        "product",
        jax.ShapeDtypeStruct(stacked, bf16),
        flops,
        own.reshape(stacked),
        other.reshape(stacked),
        right.reshape(stacked),
    )
    sums = exchange(sums.reshape(message.shape))
    place = lax.axis_index("core").astype(jnp.int32).reshape(1)
    return call(
        functools.partial(output_kernel, split),
        "output",
        jax.ShapeDtypeStruct(pair_input.shape, bf16),
        flops // 2,
        place,
        sums,
        gate,
        gains[2],
        gains[3],
        w_out,
        scalars=1,
    )


def suits(mesh, pair_input, w_proj):
    row_count, col_count, depth_count = (mesh.shape[a] for a in ("row", "col", "depth"))
    split = row_count * col_count * depth_count // 2
    rows, columns = pair_input.shape[0] // row_count, pair_input.shape[1] // (col_count * depth_count)
    return (
        depth_count % 2 == 0
        and pair_input.shape[0] == pair_input.shape[1]
        and pair_input.shape[2] == LANES
        and w_proj.shape == (LANES, 4 * LANES)
        and split & (split - 1) == 0
        and split >= 16
        and LANES % split == 0
        and rows % split == 0
        and columns % ROWS == 0
        and rows % (2 * columns) == 0
    )


def solution(mesh):
    def step(pair_input, in_gain, in_shift, w_proj, w_gate, out_gain, out_shift, w_out):
        if suits(mesh, pair_input, w_proj):
            row_count, col_count, depth_count = mesh.devices.shape
            used = Mesh(
                mesh.devices.reshape(row_count, col_count, depth_count // 2, 2),
                ("row", "col", "depth", "core"),
            )
            pair, body = P("row", ("col", "depth", "core"), None), fast_device
        else:
            used, pair, body = mesh, P("row", ("col", "depth"), None), plain_device
        return jax.shard_map(
            body,
            mesh=used,
            in_specs=(pair, P(), P(), P(), P(), P(), P(), P()),
            out_specs=pair,
            check_vma=False,
        )(pair_input, in_gain, in_shift, w_proj, w_gate, out_gain, out_shift, w_out)

    return step
```

```python
import functools

import jax
import jax.numpy as jnp
from jax import lax
from jax.experimental import pallas as pl
from jax.experimental.pallas import tpu as pltpu
from jax.sharding import Mesh
from jax.sharding import PartitionSpec as P

LANES = 128
ROWS = 8
VMEM_LIMIT = 24 * 1024 * 1024
NT = (((1,), (1,)), ((), ()))


def layer_norm(values, scaling, offsets):
    average = jnp.mean(values, axis=-1, keepdims=True)
    centred = values - average
    variance = jnp.mean(centred * centred, axis=-1, keepdims=True)
    return centred * lax.rsqrt(variance + 1e-05) * scaling + offsets


def reorder_channels(values, row_count, other_count):
    shape_rest = values.shape[1:]
    grouped = values.reshape((row_count, other_count, -1) + shape_rest)
    return jnp.swapaxes(grouped, 0, 1).reshape(values.shape)


def plain_device(pair_input, in_gain, in_shift, w_proj, w_gate, out_gain, out_shift, w_out):
    row_count = lax.axis_size("row")
    others = ("col", "depth")
    other_count = lax.axis_size("col") * lax.axis_size("depth")
    channels = w_proj.shape[1] // 4
    normed = layer_norm(pair_input.astype(jnp.float32), in_gain, in_shift).astype(jnp.bfloat16)
    projected = jnp.einsum("xyc,cd->xyd", normed, w_proj, preferred_element_type=jnp.float32)
    sides = []
    for at in (0, 2 * channels):
        gate = jax.nn.sigmoid(projected[..., at : at + channels])
        side = (gate * projected[..., at + channels : at + 2 * channels]).astype(jnp.bfloat16)
        side = lax.all_to_all(side, "row", split_axis=2, concat_axis=0, tiled=True)
        sides.append(lax.all_to_all(side, others, split_axis=2, concat_axis=1, tiled=True))
    planes = jnp.einsum("kic,kjc->ijc", *sides, preferred_element_type=jnp.float32)
    product = lax.all_to_all(
        planes.astype(jnp.bfloat16), "row", split_axis=0, concat_axis=2, tiled=True
    )
    product = lax.all_to_all(product, others, split_axis=1, concat_axis=2, tiled=True)
    used = [reorder_channels(a, row_count, other_count) for a in (out_gain, out_shift, w_out)]
    product_norm = layer_norm(product.astype(jnp.float32), used[0], used[1]).astype(jnp.bfloat16)
    gating = jax.nn.sigmoid(
        jnp.einsum("xyc,cd->xyd", normed, w_gate, preferred_element_type=jnp.float32)
    )
    out = jnp.einsum("xyc,cd->xyd", product_norm, used[2], preferred_element_type=jnp.float32)
    return (gating * out).astype(jnp.bfloat16)


def swap_with_lanes(tiles):
    tiles = list(tiles)
    count = len(tiles)
    lane = lax.broadcasted_iota(jnp.int32, tiles[0].shape, 1)
    step = 1
    while step < count:
        upper = (lane & step) != 0
        new = list(tiles)
        for v in range(count):
            if not v & step:
                low, high = tiles[v], tiles[v | step]
                new[v] = jnp.where(upper, pltpu.roll(high, step, 1), low)
                new[v | step] = jnp.where(upper, high, pltpu.roll(low, LANES - step, 1))
        tiles = new
        step *= 2
    return tiles


def side_of(normed, weights, channels):
    projected = jnp.dot(normed, weights, preferred_element_type=jnp.float32)
    return jax.nn.sigmoid(projected[:, :channels]) * projected[:, channels:]


def store_side(side, out_ref, split, k_group, i_tile):
    tiles = [side[s * ROWS : (s + 1) * ROWS] for s in range(split)]
    tiles = swap_with_lanes(tiles)
    for s in range(split):
        out_ref[
            s,
            i_tile * ROWS : (i_tile + 1) * ROWS,
            k_group * LANES : (k_group + 1) * LANES,
        ] = tiles[s].astype(out_ref.dtype)


def left_kernel(split, x_ref, gain_ref, shift_ref, w_ref, normed_ref, out_ref):
    rows, columns, channels = x_ref.shape
    for k_group in range(rows // split):
        for i_tile in range(columns // ROWS):
            at = (slice(k_group * split, (k_group + 1) * split), slice(i_tile * ROWS, (i_tile + 1) * ROWS))
            values = x_ref[at].astype(jnp.float32).reshape(split * ROWS, channels)
            normed = layer_norm(values, gain_ref[...], shift_ref[...])
            normed_ref[at] = normed.reshape(split, ROWS, channels).astype(jnp.bfloat16)
            side = side_of(normed.astype(jnp.bfloat16), w_ref[:, : 2 * channels], channels)
            store_side(side, out_ref, split, k_group, i_tile)


def right_kernel(split, normed_ref, w_ref, out_ref):
    rows, columns, channels = normed_ref.shape
    for k_group in range(rows // split):
        for i_tile in range(columns // ROWS):
            at = (slice(k_group * split, (k_group + 1) * split), slice(i_tile * ROWS, (i_tile + 1) * ROWS))
            normed = normed_ref[at].reshape(split * ROWS, channels)
            side = side_of(normed, w_ref[:, 2 * channels :], channels)
            store_side(side, out_ref, split, k_group, i_tile)


def gate_kernel(normed_ref, w_ref, out_ref):
    rows, columns, channels = normed_ref.shape
    normed = normed_ref[...].reshape(rows * columns, channels)
    gate = jax.nn.sigmoid(jnp.dot(normed, w_ref[...], preferred_element_type=jnp.float32))
    out_ref[...] = gate.reshape(rows, columns, channels)


def product_kernel(split, own_ref, other_ref, right_ref, out_ref):
    row_count, rows, width = own_ref.shape
    columns = rows // row_count
    groups = LANES // split
    right = jnp.concatenate([right_ref[r] for r in range(row_count)], axis=1)
    lane = lax.broadcasted_iota(jnp.int32, (split, row_count * width), 1)
    group = lax.rem(lane, LANES) // split
    for target in range(row_count):
        at = slice(target * columns, (target + 1) * columns)
        left = jnp.concatenate(
            [
                jnp.concatenate([ref[r, at, :] for r in range(row_count)], axis=1)
                for ref in (own_ref, other_ref)
            ],
            axis=0,
        )
        parts = []
        for slab in range(2 * columns // split):
            piece = left[slab * split : (slab + 1) * split]
            for g in range(groups):
                parts.append(jnp.where(group == g, piece, jnp.zeros_like(piece)))
        masked = jnp.concatenate(parts, axis=0)
        block = lax.dot_general(right, masked, NT, preferred_element_type=jnp.float32)
        out_ref[target] = block.astype(out_ref.dtype)


def output_kernel(split, place_ref, sums_ref, gate_ref, gain_ref, shift_ref, w_ref, out_ref):
    _, columns, width = sums_ref.shape
    rows, _, channels = out_ref.shape
    parity = place_ref[0]
    pieces = split // ROWS
    for j_tile in range(columns // ROWS):
        js = slice(j_tile * ROWS, (j_tile + 1) * ROWS)
        for slab in range(width // LANES):
            lanes = slice(slab * LANES, (slab + 1) * LANES)
            tiles = [sums_ref[s, js, lanes].astype(jnp.float32) for s in range(split)]
            tiles = swap_with_lanes(tiles)
            values = jnp.concatenate(tiles, axis=0)
            normed = layer_norm(values, gain_ref[...], shift_ref[...]).astype(jnp.bfloat16)
            projected = jnp.dot(normed, w_ref[...], preferred_element_type=jnp.float32)
            for piece in range(pieces):
                first = slab * split + piece * ROWS
                half, rest = divmod(first, rows // 2)
                block, inside = divmod(rest, columns)
                core = parity if half == 0 else 1 - parity
                at = pl.ds((2 * block + core) * columns + inside, ROWS)
                value = projected[piece * ROWS * ROWS : (piece + 1) * ROWS * ROWS]
                value = value.reshape(ROWS, ROWS, channels)
                out_ref[at, js, :] = (gate_ref[at, js, :] * value).astype(out_ref.dtype)


def call(kernel, name, out_shape, flops, *arrays, scalars=0):
    specs = [pl.BlockSpec(memory_space=pltpu.SMEM)] * scalars
    specs += [pl.BlockSpec(memory_space=pltpu.VMEM)] * (len(arrays) - scalars)
    outs = jax.tree.leaves(out_shape)
    moved = sum(a.size * a.dtype.itemsize for a in [*arrays, *outs])
    return pl.pallas_call(
        kernel,
        name=name,
        out_shape=out_shape,
        in_specs=specs,
        out_specs=jax.tree.map(lambda _: pl.BlockSpec(memory_space=pltpu.VMEM), out_shape),
        cost_estimate=pl.CostEstimate(flops=flops, bytes_accessed=moved, transcendentals=0),
        compiler_params=pltpu.CompilerParams(vmem_limit_bytes=VMEM_LIMIT),
    )(*arrays)


def fast_device(pair_input, in_gain, in_shift, w_proj, w_gate, out_gain, out_shift, w_out):
    rows, columns, channels = pair_input.shape
    row_count = lax.axis_size("row")
    owners = ("row", "col", "depth")
    split = row_count * lax.axis_size("col") * lax.axis_size("depth")
    width = rows // split * LANES
    per_row = split // row_count
    bf16 = jnp.bfloat16
    gains = [a.reshape(1, channels) for a in (in_gain, in_shift, out_gain, out_shift)]
    message = jax.ShapeDtypeStruct((split, columns, width), bf16)
    flops = 4 * rows * columns * channels * channels

    normed, left = call(
        functools.partial(left_kernel, split),
        "left",
        (jax.ShapeDtypeStruct(pair_input.shape, bf16), message),
        flops,
        pair_input,
        gains[0],
        gains[1],
        w_proj,
    )
    exchange = functools.partial(
        lax.all_to_all, axis_name=owners, split_axis=0, concat_axis=0, tiled=True
    )
    own = exchange(left)
    right = exchange(call(functools.partial(right_kernel, split), "right", message, flops, normed, w_proj))
    gate = call(gate_kernel, "gate", jax.ShapeDtypeStruct(pair_input.shape, jnp.float32), flops // 2, normed, w_gate)
    other = lax.ppermute(own, "core", [(0, 1), (1, 0)])
    stacked = (row_count, per_row * columns, width)
    sums = call(
        functools.partial(product_kernel, split),
        "product",
        jax.ShapeDtypeStruct(stacked, bf16),
        flops,
        own.reshape(stacked),
        other.reshape(stacked),
        right.reshape(stacked),
    )
    sums = exchange(sums.reshape(message.shape))
    place = lax.axis_index("core").astype(jnp.int32).reshape(1)
    return call(
        functools.partial(output_kernel, split),
        "output",
        jax.ShapeDtypeStruct(pair_input.shape, bf16),
        flops // 2,
        place,
        sums,
        gate,
        gains[2],
        gains[3],
        w_out,
        scalars=1,
    )


def suits(mesh, pair_input, w_proj):
    row_count, col_count, depth_count = (mesh.shape[a] for a in ("row", "col", "depth"))
    split = row_count * col_count * depth_count // 2
    rows, columns = pair_input.shape[0] // row_count, pair_input.shape[1] // (col_count * depth_count)
    return (
        depth_count % 2 == 0
        and pair_input.shape[0] == pair_input.shape[1]
        and pair_input.shape[2] == LANES
        and w_proj.shape == (LANES, 4 * LANES)
        and split & (split - 1) == 0
        and split >= 16
        and LANES % split == 0
        and rows % split == 0
        and columns % ROWS == 0
        and rows % (2 * columns) == 0
    )


def solution(mesh):
    def step(pair_input, in_gain, in_shift, w_proj, w_gate, out_gain, out_shift, w_out):
        if suits(mesh, pair_input, w_proj):
            row_count, col_count, depth_count = mesh.devices.shape
            used = Mesh(
                mesh.devices.reshape(row_count, col_count, depth_count // 2, 2),
                ("row", "col", "depth", "core"),
            )
            pair, body = P("row", ("col", "depth", "core"), None), fast_device
        else:
            used, pair, body = mesh, P("row", ("col", "depth"), None), plain_device
        return jax.shard_map(
            body,
            mesh=used,
            in_specs=(pair, P(), P(), P(), P(), P(), P(), P()),
            out_specs=pair,
            check_vma=False,
        )(pair_input, in_gain, in_shift, w_proj, w_gate, out_gain, out_shift, w_out)

    return step
```

```python
import functools

import jax
import jax.numpy as jnp
from jax import lax
from jax.experimental import pallas as pl
from jax.experimental.pallas import tpu as pltpu
from jax.sharding import Mesh
from jax.sharding import PartitionSpec as P

LANES = 128
ROWS = 8
VMEM_LIMIT = 24 * 1024 * 1024
NT = (((1,), (1,)), ((), ()))


def layer_norm(values, scaling, offsets):
    average = jnp.mean(values, axis=-1, keepdims=True)
    centred = values - average
    variance = jnp.mean(centred * centred, axis=-1, keepdims=True)
    return centred * lax.rsqrt(variance + 1e-05) * scaling + offsets


def reorder_channels(values, row_count, other_count):
    shape_rest = values.shape[1:]
    grouped = values.reshape((row_count, other_count, -1) + shape_rest)
    return jnp.swapaxes(grouped, 0, 1).reshape(values.shape)


def plain_device(pair_input, in_gain, in_shift, w_proj, w_gate, out_gain, out_shift, w_out):
    row_count = lax.axis_size("row")
    others = ("col", "depth")
    other_count = lax.axis_size("col") * lax.axis_size("depth")
    channels = w_proj.shape[1] // 4
    normed = layer_norm(pair_input.astype(jnp.float32), in_gain, in_shift).astype(jnp.bfloat16)
    projected = jnp.einsum("xyc,cd->xyd", normed, w_proj, preferred_element_type=jnp.float32)
    sides = []
    for at in (0, 2 * channels):
        gate = jax.nn.sigmoid(projected[..., at : at + channels])
        side = (gate * projected[..., at + channels : at + 2 * channels]).astype(jnp.bfloat16)
        side = lax.all_to_all(side, "row", split_axis=2, concat_axis=0, tiled=True)
        sides.append(lax.all_to_all(side, others, split_axis=2, concat_axis=1, tiled=True))
    planes = jnp.einsum("kic,kjc->ijc", *sides, preferred_element_type=jnp.float32)
    product = lax.all_to_all(
        planes.astype(jnp.bfloat16), "row", split_axis=0, concat_axis=2, tiled=True
    )
    product = lax.all_to_all(product, others, split_axis=1, concat_axis=2, tiled=True)
    used = [reorder_channels(a, row_count, other_count) for a in (out_gain, out_shift, w_out)]
    product_norm = layer_norm(product.astype(jnp.float32), used[0], used[1]).astype(jnp.bfloat16)
    gating = jax.nn.sigmoid(
        jnp.einsum("xyc,cd->xyd", normed, w_gate, preferred_element_type=jnp.float32)
    )
    out = jnp.einsum("xyc,cd->xyd", product_norm, used[2], preferred_element_type=jnp.float32)
    return (gating * out).astype(jnp.bfloat16)


def spread(tiles):
    count = len(tiles)
    lane = lax.broadcasted_iota(jnp.int32, tiles[0].shape, 1)
    picked = [tiles[-v % count] for v in range(count)]
    step = 1
    while step < count:
        upper = (lane & step) != 0
        picked = [jnp.where(upper, picked[v - step], picked[v]) for v in range(count)]
        step *= 2
    return picked


def turn(tile, lanes):
    return pltpu.roll(tile, lanes % LANES, 1) if lanes % LANES else tile


def edges_kernel(
    split, x_hbm, gain_hbm, shift_hbm, w_hbm, wg_hbm, og_hbm, os_hbm, wo_hbm,
    out_ref, normed_ref, wg_ref, og_ref, os_ref, wo_ref, x_ref, gain_ref, shift_ref, w_ref, sems,
):
    rows, columns, channels = x_hbm.shape
    pairs = (
        (x_hbm, x_ref), (gain_hbm, gain_ref), (shift_hbm, shift_ref), (w_hbm, w_ref),
        (wg_hbm, wg_ref), (og_hbm, og_ref), (os_hbm, os_ref), (wo_hbm, wo_ref),
    )
    copies = [pltpu.make_async_copy(a, b, sems.at[n]) for n, (a, b) in enumerate(pairs)]
    for copy in copies:
        copy.start()
    for copy in copies[:4]:
        copy.wait()
    for k_group in range(rows // split):
        for i_tile in range(columns // ROWS):
            at = (slice(k_group * split, (k_group + 1) * split), slice(i_tile * ROWS, (i_tile + 1) * ROWS))
            values = x_ref[at].astype(jnp.float32).reshape(split * ROWS, channels)
            normed = layer_norm(values, gain_ref[...], shift_ref[...])
            normed_ref[at] = normed.reshape(split, ROWS, channels).astype(jnp.bfloat16)
            projected = jnp.dot(
                normed.astype(jnp.bfloat16), w_ref[...], preferred_element_type=jnp.float32
            )
            for side in range(2):
                gate = projected[:, 2 * side * channels : (2 * side + 1) * channels]
                value = projected[:, (2 * side + 1) * channels : (2 * side + 2) * channels]
                edge = jax.nn.sigmoid(gate) * value
                tiles = [turn(edge[k * ROWS : (k + 1) * ROWS], k) for k in range(split)]
                for s, tile in enumerate(spread(tiles)):
                    first = side * columns + i_tile * ROWS
                    out_ref[
                        s, first : first + ROWS, k_group * LANES : (k_group + 1) * LANES
                    ] = tile.astype(out_ref.dtype)
    for copy in copies[4:]:
        copy.wait()


def side_by_side(ref, at):
    return jnp.concatenate([ref[r, at, :] for r in range(ref.shape[0])], axis=1)


def group_masks(split, place, width):
    lane = lax.broadcasted_iota(jnp.int32, (split, LANES), 1)
    group = lax.shift_right_logical(
        (lane - place) & (LANES - 1), jnp.int32(split.bit_length() - 1)
    )
    return [
        jnp.concatenate([(group == g).astype(jnp.bfloat16)] * (width // LANES), axis=1)
        for g in range(LANES // split)
    ]


def slab_products(right, slab, masks):
    masked = jnp.concatenate([slab * mask for mask in masks], axis=0)
    return lax.dot_general(right, masked, NT, preferred_element_type=jnp.float32)


def pieces_of(split, columns, row_blocks):
    firsts = list(range(0, row_blocks * columns, ROWS))
    per = split // ROWS
    whole = len(firsts) // per * per
    order = [(core, first) for core in (0, 1) for first in firsts[:whole]]
    order += [(core, first) for core in (0, 1) for first in firsts[whole:]]
    return [order[n : n + per] for n in range(0, len(order), per)]


def own_kernel(split, place_ref, own_ref, right_ref, normed_ref, wg_ref, out_ref, gate_ref):
    row_count, rows, width = own_ref.shape
    columns = rows // row_count
    right = side_by_side(right_ref, slice(None))
    place = lax.shift_right_logical(place_ref[0], 1)
    masks = group_masks(split, place, row_count * width)
    for target in range(row_count):
        for slab in range(out_ref.shape[1]):
            first = target * columns + slab * split
            left = side_by_side(own_ref, slice(first, first + split))
            out_ref[target, slab] = slab_products(right, left, masks).astype(out_ref.dtype)
    rows, columns, channels = normed_ref.shape
    normed = normed_ref[...].reshape(rows * columns, channels)
    gate = jax.nn.sigmoid(jnp.dot(normed, wg_ref[...], preferred_element_type=jnp.float32))
    gate_ref[...] = gate.reshape(rows, columns, channels)


def other_kernel(split, slabs, place_ref, done_ref, own_ref, other_ref, right_ref, out_ref):
    row_count, rows, width = own_ref.shape
    columns = rows // row_count
    right = side_by_side(right_ref, slice(None))
    place = lax.shift_right_logical(place_ref[0], 1)
    masks = group_masks(split, place, row_count * width)
    refs = (own_ref, other_ref)
    for target in range(row_count):
        for n, slab in enumerate(slabs):
            lanes = slice(n * LANES, (n + 1) * LANES)
            if n < done_ref.shape[1]:
                out_ref[target, :, lanes] = done_ref[target, n]
                continue
            left = jnp.concatenate(
                [
                    side_by_side(refs[core], slice(target * columns + first, target * columns + first + ROWS))
                    for core, first in slab
                ],
                axis=0,
            )
            out_ref[target, :, lanes] = slab_products(right, left, masks).astype(out_ref.dtype)


def output_kernel(split, slabs, place_ref, sums_ref, gate_ref, gain_ref, shift_ref, w_ref, out_ref):
    columns = sums_ref.shape[1]
    channels = out_ref.shape[2]
    parity = place_ref[0] & 1
    for j_tile in range(columns // ROWS):
        js = slice(j_tile * ROWS, (j_tile + 1) * ROWS)
        for n, slab in enumerate(slabs):
            lanes = slice(n * LANES, (n + 1) * LANES)
            tiles = [turn(sums_ref[s, js, lanes].astype(jnp.float32), s) for s in range(split)]
            tiles = [turn(tile, -i) for i, tile in enumerate(spread(tiles))]
            values = jnp.concatenate(tiles, axis=0)
            normed = layer_norm(values, gain_ref[...], shift_ref[...]).astype(jnp.bfloat16)
            projected = jnp.dot(normed, w_ref[...], preferred_element_type=jnp.float32)
            for piece, (core, first) in enumerate(slab):
                block, inside = divmod(first, columns)
                core = parity if core == 0 else 1 - parity
                at = pl.ds((2 * block + core) * columns + inside, ROWS)
                value = projected[piece * ROWS * ROWS : (piece + 1) * ROWS * ROWS]
                value = value.reshape(ROWS, ROWS, channels)
                out_ref[at, js, :] = (gate_ref[at, js, :] * value).astype(out_ref.dtype)


SMEM = pl.BlockSpec(memory_space=pltpu.SMEM)
VMEM = pl.BlockSpec(memory_space=pltpu.VMEM)
HBM = pl.BlockSpec(memory_space=pltpu.HBM)


def call(kernel, name, out_shape, specs, flops, *arrays, scratch=()):
    outs = jax.tree.leaves(out_shape)
    moved = sum(a.size * a.dtype.itemsize for a in [*arrays, *outs])
    return pl.pallas_call(
        kernel,
        name=name,
        out_shape=out_shape,
        in_specs=specs,
        out_specs=jax.tree.map(lambda _: VMEM, out_shape),
        scratch_shapes=scratch,
        cost_estimate=pl.CostEstimate(flops=flops, bytes_accessed=moved, transcendentals=0),
        compiler_params=pltpu.CompilerParams(vmem_limit_bytes=VMEM_LIMIT),
    )(*arrays)


def fast_device(pair_input, in_gain, in_shift, w_proj, w_gate, out_gain, out_shift, w_out):
    rows, columns, channels = pair_input.shape
    row_count = lax.axis_size("row")
    owners = ("row", "col", "depth")
    split = row_count * lax.axis_size("col") * lax.axis_size("depth")
    width = rows // split * LANES
    per_row = split // row_count
    slabs = pieces_of(split, columns, rows // (2 * columns))
    own_slabs = sum(all(core == 0 for core, _ in slab) for slab in slabs)
    bf16, f32 = jnp.bfloat16, jnp.float32
    shape = jax.ShapeDtypeStruct
    gains = [a.reshape(1, channels) for a in (in_gain, in_shift, out_gain, out_shift)]
    flops = 4 * rows * columns * channels * channels
    place = lax.axis_index(("row", "col", "depth", "core")).astype(jnp.int32).reshape(1)

    edges, normed, wg, og, os, wo = call(
        functools.partial(edges_kernel, split),
        "edges",
        (
            shape((split, 2 * columns, width), bf16),
            shape(pair_input.shape, bf16),
            shape(w_gate.shape, bf16),
            shape((1, channels), f32),
            shape((1, channels), f32),
            shape(w_out.shape, bf16),
        ),
        [HBM] * 8,
        2 * flops,
        *(
            pltpu.with_memory_space_constraint(a, pltpu.HBM)
            for a in (pair_input, gains[0], gains[1], w_proj, w_gate, gains[2], gains[3], w_out)
        ),
        scratch=(
            pltpu.VMEM(pair_input.shape, bf16),
            pltpu.VMEM((1, channels), f32),
            pltpu.VMEM((1, channels), f32),
            pltpu.VMEM(w_proj.shape, bf16),
            pltpu.SemaphoreType.DMA((8,)),
        ),
    )
    exchange = functools.partial(
        lax.all_to_all, axis_name=owners, split_axis=0, concat_axis=0, tiled=True
    )
    edges = exchange(edges)
    own, right = edges[:, :columns], edges[:, columns:]
    other = lax.ppermute(own, "core", [(0, 1), (1, 0)])
    stacked = (row_count, per_row * columns, width)
    own, other, right = (a.reshape(stacked) for a in (own, other, right))
    done, gate = call(
        functools.partial(own_kernel, split),
        "own",
        (
            shape((row_count, own_slabs, per_row * columns, LANES), bf16),
            shape(pair_input.shape, f32),
        ),
        [SMEM] + [VMEM] * 4,
        flops,
        place, own, right, normed, wg,
    )
    sums = call(
        functools.partial(other_kernel, split, slabs),
        "other",
        shape(stacked, bf16),
        [SMEM] + [VMEM] * 4,
        flops,
        place, done, own, other, right,
    )
    sums = exchange(sums.reshape(split, columns, width))
    return call(
        functools.partial(output_kernel, split, slabs),
        "output",
        shape(pair_input.shape, bf16),
        [SMEM] + [VMEM] * 5,
        flops // 2,
        place, sums, gate, og, os, wo,
    )


def suits(mesh, pair_input, w_proj):
    row_count, col_count, depth_count = (mesh.shape[a] for a in ("row", "col", "depth"))
    split = row_count * col_count * depth_count // 2
    rows, columns = pair_input.shape[0] // row_count, pair_input.shape[1] // (col_count * depth_count)
    return (
        depth_count % 2 == 0
        and pair_input.shape[0] == pair_input.shape[1]
        and pair_input.shape[2] == LANES
        and w_proj.shape == (LANES, 4 * LANES)
        and split & (split - 1) == 0
        and split >= 16
        and LANES % split == 0
        and rows % split == 0
        and columns % ROWS == 0
        and rows % (2 * columns) == 0
    )


def solution(mesh):
    def step(pair_input, in_gain, in_shift, w_proj, w_gate, out_gain, out_shift, w_out):
        if suits(mesh, pair_input, w_proj):
            row_count, col_count, depth_count = mesh.devices.shape
            used = Mesh(
                mesh.devices.reshape(row_count, col_count, depth_count // 2, 2),
                ("row", "col", "depth", "core"),
            )
            pair, body = P("row", ("col", "depth", "core"), None), fast_device
        else:
            used, pair, body = mesh, P("row", ("col", "depth"), None), plain_device
        return jax.shard_map(
            body,
            mesh=used,
            in_specs=(pair, P(), P(), P(), P(), P(), P(), P()),
            out_specs=pair,
            check_vma=False,
        )(pair_input, in_gain, in_shift, w_proj, w_gate, out_gain, out_shift, w_out)

    return step
```

```python
import functools

import jax
import jax.numpy as jnp
from jax import lax
from jax.experimental import pallas as pl
from jax.experimental.pallas import tpu as pltpu
from jax.sharding import Mesh
from jax.sharding import PartitionSpec as P

LANES = 128
ROWS = 8
VMEM_LIMIT = 24 * 1024 * 1024
NT = (((1,), (1,)), ((), ()))


def layer_norm(values, scaling, offsets):
    average = jnp.mean(values, axis=-1, keepdims=True)
    centred = values - average
    variance = jnp.mean(centred * centred, axis=-1, keepdims=True)
    return centred * lax.rsqrt(variance + 1e-05) * scaling + offsets


def reorder_channels(values, row_count, other_count):
    shape_rest = values.shape[1:]
    grouped = values.reshape((row_count, other_count, -1) + shape_rest)
    return jnp.swapaxes(grouped, 0, 1).reshape(values.shape)


def plain_device(pair_input, in_gain, in_shift, w_proj, w_gate, out_gain, out_shift, w_out):
    row_count = lax.axis_size("row")
    others = ("col", "depth")
    other_count = lax.axis_size("col") * lax.axis_size("depth")
    channels = w_proj.shape[1] // 4
    normed = layer_norm(pair_input.astype(jnp.float32), in_gain, in_shift).astype(jnp.bfloat16)
    projected = jnp.einsum("xyc,cd->xyd", normed, w_proj, preferred_element_type=jnp.float32)
    sides = []
    for at in (0, 2 * channels):
        gate = jax.nn.sigmoid(projected[..., at : at + channels])
        side = (gate * projected[..., at + channels : at + 2 * channels]).astype(jnp.bfloat16)
        side = lax.all_to_all(side, "row", split_axis=2, concat_axis=0, tiled=True)
        sides.append(lax.all_to_all(side, others, split_axis=2, concat_axis=1, tiled=True))
    planes = jnp.einsum("kic,kjc->ijc", *sides, preferred_element_type=jnp.float32)
    product = lax.all_to_all(
        planes.astype(jnp.bfloat16), "row", split_axis=0, concat_axis=2, tiled=True
    )
    product = lax.all_to_all(product, others, split_axis=1, concat_axis=2, tiled=True)
    used = [reorder_channels(a, row_count, other_count) for a in (out_gain, out_shift, w_out)]
    product_norm = layer_norm(product.astype(jnp.float32), used[0], used[1]).astype(jnp.bfloat16)
    gating = jax.nn.sigmoid(
        jnp.einsum("xyc,cd->xyd", normed, w_gate, preferred_element_type=jnp.float32)
    )
    out = jnp.einsum("xyc,cd->xyd", product_norm, used[2], preferred_element_type=jnp.float32)
    return (gating * out).astype(jnp.bfloat16)


def spread(tiles):
    count = len(tiles)
    lane = lax.broadcasted_iota(jnp.int32, tiles[0].shape, 1)
    picked = [tiles[-v % count] for v in range(count)]
    step = 1
    while step < count:
        upper = (lane & step) != 0
        picked = [jnp.where(upper, picked[v - step], picked[v]) for v in range(count)]
        step *= 2
    return picked


def turn(tile, lanes):
    return pltpu.roll(tile, lanes % LANES, 1) if lanes % LANES else tile


def kernel_norm(values, scaling, offsets):
    share = jnp.full((LANES, LANES), 1 / LANES, jnp.bfloat16)
    centred = values.astype(jnp.float32) - jnp.dot(values, share, preferred_element_type=jnp.float32)
    variance = jnp.mean(centred * centred, axis=-1, keepdims=True)
    return (centred * lax.rsqrt(variance + 1e-05) * scaling + offsets).astype(jnp.bfloat16)


def edges_kernel(
    split, x_hbm, gain_hbm, shift_hbm, w_hbm, wg_hbm, og_hbm, os_hbm, wo_hbm,
    out_ref, normed_ref, wg_ref, og_ref, os_ref, wo_ref, x_ref, gain_ref, shift_ref, w_ref, sems,
):
    rows, columns, channels = x_hbm.shape
    pairs = (
        (x_hbm, x_ref), (gain_hbm, gain_ref), (shift_hbm, shift_ref), (w_hbm, w_ref),
        (wg_hbm, wg_ref), (og_hbm, og_ref), (os_hbm, os_ref), (wo_hbm, wo_ref),
    )
    copies = [pltpu.make_async_copy(a, b, sems.at[n]) for n, (a, b) in enumerate(pairs)]
    for copy in copies:
        copy.start()
    for copy in copies[:4]:
        copy.wait()
    normed = []
    for slab in range(rows // split):
        ks = slice(slab * split, (slab + 1) * split)
        values = x_ref[ks].reshape(split * columns, channels)
        normed.append(kernel_norm(values, gain_ref[...], shift_ref[...]))
        normed_ref[ks] = normed[-1].reshape(split, columns, channels)
    for slab, values in enumerate(normed):
        projected = jnp.dot(values, w_ref[...], preferred_element_type=jnp.float32)
        for i_tile in range(columns // ROWS):
            tiles = []
            for k in range(split):
                first = k * columns + i_tile * ROWS
                part = projected[first : first + ROWS]
                parts = [part[:, n * channels : (n + 1) * channels] for n in range(4)]
                left = jax.nn.sigmoid(parts[0]) * parts[1]
                right = jax.nn.sigmoid(parts[2]) * parts[3]
                both = jnp.concatenate([left, right], axis=0).astype(out_ref.dtype)
                tiles.append(turn(both, k))
            for s, tile in enumerate(spread(tiles)):
                at = slice(2 * i_tile * ROWS, 2 * (i_tile + 1) * ROWS)
                out_ref[s, at, slab * LANES : (slab + 1) * LANES] = tile
    for copy in copies[4:]:
        copy.wait()


def place_in(*axes):
    place = lax.axis_index(axes[0])
    for axis in axes[1:]:
        place = place * lax.axis_size(axis) + lax.axis_index(axis)
    return place


def lane_place(shape, place):
    return (lax.broadcasted_iota(jnp.int32, shape, 1) - place) & (LANES - 1)


def k_tiles(ref, at):
    return [
        ref[r, at, t * LANES : (t + 1) * LANES]
        for r in range(ref.shape[0])
        for t in range(ref.shape[2] // LANES)
    ]


def fold(tiles, place):
    low = lane_place(tiles[0].shape, place) < LANES // 2
    halves = ([], [])
    for first, second in zip(tiles[::2], tiles[1::2]):
        halves[0].append(jnp.where(low, first, turn(second, LANES // 2)))
        halves[1].append(jnp.where(low, turn(first, LANES // 2), second))
    return [jnp.concatenate(half, axis=1) for half in halves]


def slab_products(split, place, rights, units):
    groups = LANES // split // 2
    shift = split.bit_length() - 1
    position = lane_place((split, LANES), place)
    group = lax.shift_right_logical(position, jnp.int32(shift)) & (groups - 1)
    count = rights[0].shape[1] // LANES
    masks = [
        jnp.concatenate([(group == g).astype(jnp.bfloat16)] * count, axis=1) for g in range(groups)
    ]
    masked = ([], [])
    for unit in units:
        for half, folded in enumerate(fold(unit, place)):
            masked[half].extend(folded * mask for mask in masks)
    low, high = (
        lax.dot_general(
            right, jnp.concatenate(parts, axis=0), NT, preferred_element_type=jnp.float32
        ).astype(jnp.bfloat16)
        for right, parts in zip(rights, masked)
    )
    first_half = lax.broadcasted_iota(jnp.int32, (rights[0].shape[0], LANES), 1) < LANES // 2
    out = []
    for n in range(0, len(units) * LANES // 2, LANES):
        lows, highs = low[:, n : n + LANES], high[:, n : n + LANES]
        out.append(jnp.where(first_half, lows, turn(highs, LANES // 2)))
        out.append(jnp.where(first_half, turn(lows, LANES // 2), highs))
    return out


def pieces_of(split, columns, row_blocks):
    firsts = list(range(0, row_blocks * columns, ROWS))
    per = split // ROWS
    whole = len(firsts) // per * per
    order = [(core, first) for core in (0, 1) for first in firsts[:whole]]
    order += [(core, first) for core in (0, 1) for first in firsts[whole:]]
    return [order[n : n + per] for n in range(0, len(order), per)]


def own_kernel(split, own_ref, right_ref, normed_ref, wg_ref, out_ref, gate_ref, rights_ref):
    row_count, rows, _ = own_ref.shape
    columns = rows // row_count
    place = place_in("row", "col", "depth")
    rights = fold(k_tiles(right_ref, slice(None)), place)
    for half in range(2):
        rights_ref[half] = rights[half]
    slots = [(target, slab) for target in range(row_count) for slab in range(out_ref.shape[1])]
    units = []
    for target, slab in slots:
        first = target * columns + slab * split
        units.append(k_tiles(own_ref, slice(first, first + split)))
    for (target, slab), block in zip(slots, slab_products(split, place, rights, units)):
        out_ref[target, slab] = block
    rows, columns, channels = normed_ref.shape
    normed = normed_ref[...].reshape(rows * columns, channels)
    gate = jax.nn.sigmoid(jnp.dot(normed, wg_ref[...], preferred_element_type=jnp.float32))
    gate_ref[...] = gate.reshape(rows, columns, channels)


def other_kernel(split, slabs, done_ref, own_ref, other_ref, rights_ref, out_ref):
    row_count, rows, _ = own_ref.shape
    columns = rows // row_count
    place = place_in("row", "col", "depth")
    rights = [rights_ref[half] for half in range(2)]
    refs = (own_ref, other_ref)
    done = done_ref.shape[1]
    for start in range(0, row_count, 2):
        slots, units = [], []
        for target in (start, start + 1):
            for slab in range(done):
                out_ref[target, :, slab * LANES : (slab + 1) * LANES] = done_ref[target, slab]
            for slab in range(done, len(slabs)):
                pieces = [
                    k_tiles(refs[core], slice(target * columns + first, target * columns + first + ROWS))
                    for core, first in slabs[slab]
                ]
                slots.append((target, slab))
                units.append([jnp.concatenate(parts, axis=0) for parts in zip(*pieces)])
        for (target, slab), block in zip(slots, slab_products(split, place, rights, units)):
            out_ref[target, :, slab * LANES : (slab + 1) * LANES] = block


def output_kernel(split, slabs, sums_ref, gate_ref, gain_ref, shift_ref, w_ref, out_ref):
    columns = sums_ref.shape[1]
    channels = out_ref.shape[2]
    parity = lax.axis_index("core")

    def finish(tiles, n, js):
        normed = kernel_norm(jnp.concatenate(tiles, axis=0), gain_ref[...], shift_ref[...])
        projected = jnp.dot(normed, w_ref[...], preferred_element_type=jnp.float32)
        for piece, (core, first) in enumerate(slabs[n]):
            block, inside = divmod(first, columns)
            core = parity if core == 0 else 1 - parity
            at = pl.ds((2 * block + core) * columns + inside, ROWS)
            value = projected[piece * ROWS * ROWS : (piece + 1) * ROWS * ROWS]
            value = value.reshape(ROWS, ROWS, channels)
            out_ref[at, js, :] = (gate_ref[at, js, :] * value).astype(out_ref.dtype)

    units = [
        (n, slice(first, first + ROWS)) for n in range(len(slabs)) for first in range(0, columns, ROWS)
    ]
    for start in range(0, len(units), 2):
        both = units[start : start + 2]
        tiles = []
        for s in range(split):
            parts = [sums_ref[s, js, n * LANES : (n + 1) * LANES] for n, js in both]
            tiles.append(turn(jnp.concatenate(parts, axis=0), s))
        tiles = [turn(tile, -i) for i, tile in enumerate(spread(tiles))]
        for at, (n, js) in enumerate(both):
            finish([tile[at * ROWS : (at + 1) * ROWS] for tile in tiles], n, js)


VMEM = pl.BlockSpec(memory_space=pltpu.VMEM)
HBM = pl.BlockSpec(memory_space=pltpu.HBM)


def call(kernel, name, out_shape, specs, flops, *arrays, scratch=()):
    outs = jax.tree.leaves(out_shape)
    moved = sum(a.size * a.dtype.itemsize for a in [*arrays, *outs])
    return pl.pallas_call(
        kernel,
        name=name,
        out_shape=out_shape,
        in_specs=specs,
        out_specs=jax.tree.map(lambda _: VMEM, out_shape),
        scratch_shapes=scratch,
        cost_estimate=pl.CostEstimate(flops=flops, bytes_accessed=moved, transcendentals=0),
        compiler_params=pltpu.CompilerParams(vmem_limit_bytes=VMEM_LIMIT),
    )(*arrays)


def fast_device(pair_input, in_gain, in_shift, w_proj, w_gate, out_gain, out_shift, w_out):
    rows, columns, channels = pair_input.shape
    row_count = lax.axis_size("row")
    owners = ("row", "col", "depth")
    split = row_count * lax.axis_size("col") * lax.axis_size("depth")
    width = rows // split * LANES
    per_row = split // row_count
    slabs = pieces_of(split, columns, rows // (2 * columns))
    own_slabs = sum(all(core == 0 for core, _ in slab) for slab in slabs)
    bf16, f32 = jnp.bfloat16, jnp.float32
    shape = jax.ShapeDtypeStruct
    gains = [a.reshape(1, channels) for a in (in_gain, in_shift, out_gain, out_shift)]
    flops = 4 * rows * columns * channels * channels

    edges, normed, wg, og, os, wo = call(
        functools.partial(edges_kernel, split),
        "edges",
        (
            shape((split, 2 * columns, width), bf16),
            shape(pair_input.shape, bf16),
            shape(w_gate.shape, bf16),
            shape((1, channels), f32),
            shape((1, channels), f32),
            shape(w_out.shape, bf16),
        ),
        [HBM] * 8,
        2 * flops,
        *(
            pltpu.with_memory_space_constraint(a, pltpu.HBM)
            for a in (pair_input, gains[0], gains[1], w_proj, w_gate, gains[2], gains[3], w_out)
        ),
        scratch=(
            pltpu.VMEM(pair_input.shape, bf16),
            pltpu.VMEM((1, channels), f32),
            pltpu.VMEM((1, channels), f32),
            pltpu.VMEM(w_proj.shape, bf16),
            pltpu.SemaphoreType.DMA((8,)),
        ),
    )
    exchange = functools.partial(
        lax.all_to_all, axis_name=owners, split_axis=0, concat_axis=0, tiled=True
    )
    edges = exchange(edges)
    edges = edges.reshape(split, columns // ROWS, 2, ROWS, width)
    own, right = (edges[:, :, side].reshape(split, columns, width) for side in range(2))
    other = lax.ppermute(own, "core", [(0, 1), (1, 0)])
    stacked = (row_count, per_row * columns, width)
    own, other, right = (a.reshape(stacked) for a in (own, other, right))
    done, gate, rights = call(
        functools.partial(own_kernel, split),
        "own",
        (
            shape((row_count, own_slabs, per_row * columns, LANES), bf16),
            shape(pair_input.shape, f32),
            shape((2, per_row * columns, row_count * width // 2), bf16),
        ),
        [VMEM] * 4,
        flops,
        own, right, normed, wg,
    )
    sums = call(
        functools.partial(other_kernel, split, slabs),
        "other",
        shape(stacked, bf16),
        [VMEM] * 4,
        flops,
        done, own, other, rights,
    )
    sums = exchange(sums.reshape(split, columns, width))
    return call(
        functools.partial(output_kernel, split, slabs),
        "output",
        shape(pair_input.shape, bf16),
        [VMEM] * 5,
        flops // 2,
        sums, gate, og, os, wo,
    )


def suits(mesh, pair_input, w_proj):
    row_count, col_count, depth_count = (mesh.shape[a] for a in ("row", "col", "depth"))
    split = row_count * col_count * depth_count // 2
    rows, columns = pair_input.shape[0] // row_count, pair_input.shape[1] // (col_count * depth_count)
    return (
        depth_count % 2 == 0
        and pair_input.shape[0] == pair_input.shape[1]
        and pair_input.shape[2] == LANES
        and w_proj.shape == (LANES, 4 * LANES)
        and split & (split - 1) == 0
        and split >= 16
        and LANES % (2 * split) == 0
        and row_count % 2 == 0
        and rows % split == 0
        and columns % ROWS == 0
        and rows % (2 * columns) == 0
    )


def solution(mesh):
    def step(pair_input, in_gain, in_shift, w_proj, w_gate, out_gain, out_shift, w_out):
        if suits(mesh, pair_input, w_proj):
            row_count, col_count, depth_count = mesh.devices.shape
            used = Mesh(
                mesh.devices.reshape(row_count, col_count, depth_count // 2, 2),
                ("row", "col", "depth", "core"),
            )
            pair, body = P("row", ("col", "depth", "core"), None), fast_device
        else:
            used, pair, body = mesh, P("row", ("col", "depth"), None), plain_device
        return jax.shard_map(
            body,
            mesh=used,
            in_specs=(pair, P(), P(), P(), P(), P(), P(), P()),
            out_specs=pair,
            check_vma=False,
        )(pair_input, in_gain, in_shift, w_proj, w_gate, out_gain, out_shift, w_out)

    return step
```

```python
import functools

import jax
import jax.numpy as jnp
from jax import lax
from jax.experimental import pallas as pl
from jax.experimental.pallas import tpu as pltpu
from jax.sharding import Mesh
from jax.sharding import PartitionSpec as P

LANES = 128
ROWS = 8
VMEM_LIMIT = 24 * 1024 * 1024
NT = (((1,), (1,)), ((), ()))


def layer_norm(values, scaling, offsets):
    average = jnp.mean(values, axis=-1, keepdims=True)
    centred = values - average
    variance = jnp.mean(centred * centred, axis=-1, keepdims=True)
    return centred * lax.rsqrt(variance + 1e-05) * scaling + offsets


def reorder_channels(values, row_count, other_count):
    shape_rest = values.shape[1:]
    grouped = values.reshape((row_count, other_count, -1) + shape_rest)
    return jnp.swapaxes(grouped, 0, 1).reshape(values.shape)


def plain_device(pair_input, in_gain, in_shift, w_proj, w_gate, out_gain, out_shift, w_out):
    row_count = lax.axis_size("row")
    others = ("col", "depth")
    other_count = lax.axis_size("col") * lax.axis_size("depth")
    channels = w_proj.shape[1] // 4
    normed = layer_norm(pair_input.astype(jnp.float32), in_gain, in_shift).astype(jnp.bfloat16)
    projected = jnp.einsum("xyc,cd->xyd", normed, w_proj, preferred_element_type=jnp.float32)
    sides = []
    for at in (0, 2 * channels):
        gate = jax.nn.sigmoid(projected[..., at : at + channels])
        side = (gate * projected[..., at + channels : at + 2 * channels]).astype(jnp.bfloat16)
        side = lax.all_to_all(side, "row", split_axis=2, concat_axis=0, tiled=True)
        sides.append(lax.all_to_all(side, others, split_axis=2, concat_axis=1, tiled=True))
    planes = jnp.einsum("kic,kjc->ijc", *sides, preferred_element_type=jnp.float32)
    product = lax.all_to_all(
        planes.astype(jnp.bfloat16), "row", split_axis=0, concat_axis=2, tiled=True
    )
    product = lax.all_to_all(product, others, split_axis=1, concat_axis=2, tiled=True)
    used = [reorder_channels(a, row_count, other_count) for a in (out_gain, out_shift, w_out)]
    product_norm = layer_norm(product.astype(jnp.float32), used[0], used[1]).astype(jnp.bfloat16)
    gating = jax.nn.sigmoid(
        jnp.einsum("xyc,cd->xyd", normed, w_gate, preferred_element_type=jnp.float32)
    )
    out = jnp.einsum("xyc,cd->xyd", product_norm, used[2], preferred_element_type=jnp.float32)
    return (gating * out).astype(jnp.bfloat16)


def spread(tiles):
    count = len(tiles)
    lane = lax.broadcasted_iota(jnp.int32, tiles[0].shape, 1)
    picked = [tiles[-v % count] for v in range(count)]
    step = 1
    while step < count:
        upper = (lane & step) != 0
        picked = [jnp.where(upper, picked[v - step], picked[v]) for v in range(count)]
        step *= 2
    return picked


def turn(tile, lanes):
    return pltpu.roll(tile, lanes % LANES, 1) if lanes % LANES else tile


def kernel_norm(values, scaling, offsets):
    share = jnp.full((LANES, LANES), 1 / LANES, jnp.bfloat16)
    centred = values.astype(jnp.float32) - jnp.dot(values, share, preferred_element_type=jnp.float32)
    variance = jnp.mean(centred * centred, axis=-1, keepdims=True)
    return (centred * lax.rsqrt(variance + 1e-05) * scaling + offsets).astype(jnp.bfloat16)


def edges_kernel(
    split, x_hbm, gain_hbm, shift_hbm, w_hbm, wg_hbm, og_hbm, os_hbm, wo_hbm,
    out_ref, normed_ref, wg_ref, og_ref, os_ref, wo_ref, x_ref, gain_ref, shift_ref, w_ref, sems,
):
    core = lax.axis_index("core")
    rows, columns, channels = x_hbm.shape
    pairs = (
        (x_hbm, x_ref), (gain_hbm, gain_ref), (shift_hbm, shift_ref), (w_hbm, w_ref),
        (wg_hbm, wg_ref), (og_hbm, og_ref), (os_hbm, os_ref), (wo_hbm, wo_ref),
    )
    copies = [pltpu.make_async_copy(a, b, sems.at[n]) for n, (a, b) in enumerate(pairs)]
    for copy in copies:
        copy.start()
    for copy in copies[:4]:
        copy.wait()
    normed = []
    for slab in range(rows // split):
        ks = slice(slab * split, (slab + 1) * split)
        values = x_ref[ks].reshape(split * columns, channels)
        normed.append(kernel_norm(values, gain_ref[...], shift_ref[...]))
        normed_ref[ks] = normed[-1].reshape(split, columns, channels)
    for slab, values in enumerate(normed):
        projected = jnp.dot(values, w_ref[...], preferred_element_type=jnp.float32)
        for i_tile in range(columns // ROWS):
            tiles = []
            for k in range(split):
                first = k * columns + i_tile * ROWS
                part = projected[first : first + ROWS]
                parts = [part[:, n * channels : (n + 1) * channels] for n in range(4)]
                left = jax.nn.sigmoid(parts[0]) * parts[1]
                right = jax.nn.sigmoid(parts[2]) * parts[3]
                both = jnp.concatenate([left, right], axis=0).astype(out_ref.dtype)
                tiles.append(turn(both, k))
            for s, tile in enumerate(spread(tiles)):
                at = slice(i_tile * ROWS, (i_tile + 1) * ROWS)
                lanes = slice(slab * LANES, (slab + 1) * LANES)
                out_ref[s, 1 - core, at, lanes] = tile[:ROWS]
                out_ref[s, core, at, lanes] = tile[ROWS:]
    for copy in copies[4:]:
        copy.wait()


def place_in(*axes):
    place = lax.axis_index(axes[0])
    for axis in axes[1:]:
        place = place * lax.axis_size(axis) + lax.axis_index(axis)
    return place


def lane_place(shape, place):
    return (lax.broadcasted_iota(jnp.int32, shape, 1) - place) & (LANES - 1)


def k_tiles(ref, at):
    return [
        ref[r, at, t * LANES : (t + 1) * LANES]
        for r in range(ref.shape[0])
        for t in range(ref.shape[2] // LANES)
    ]


def fold(tiles, place):
    low = lane_place(tiles[0].shape, place) < LANES // 2
    halves = ([], [])
    for first, second in zip(tiles[::2], tiles[1::2]):
        halves[0].append(jnp.where(low, first, turn(second, LANES // 2)))
        halves[1].append(jnp.where(low, turn(first, LANES // 2), second))
    return [jnp.concatenate(half, axis=1) for half in halves]


def slab_products(split, place, rights, units):
    groups = LANES // split // 2
    shift = split.bit_length() - 1
    position = lane_place((split, LANES), place)
    group = lax.shift_right_logical(position, jnp.int32(shift)) & (groups - 1)
    count = rights[0].shape[1] // LANES
    masks = [
        jnp.concatenate([(group == g).astype(jnp.bfloat16)] * count, axis=1) for g in range(groups)
    ]
    masked = ([], [])
    for unit in units:
        for half, folded in enumerate(fold(unit, place)):
            masked[half].extend(folded * mask for mask in masks)
    low, high = (
        lax.dot_general(
            right, jnp.concatenate(parts, axis=0), NT, preferred_element_type=jnp.float32
        ).astype(jnp.bfloat16)
        for right, parts in zip(rights, masked)
    )
    first_half = lax.broadcasted_iota(jnp.int32, (rights[0].shape[0], LANES), 1) < LANES // 2
    out = []
    for n in range(0, len(units) * LANES // 2, LANES):
        lows, highs = low[:, n : n + LANES], high[:, n : n + LANES]
        out.append(jnp.where(first_half, lows, turn(highs, LANES // 2)))
        out.append(jnp.where(first_half, turn(lows, LANES // 2), highs))
    return out


def pieces_of(split, columns, row_blocks):
    firsts = list(range(0, row_blocks * columns, ROWS))
    per = split // ROWS
    whole = len(firsts) // per * per
    order = [(core, first) for core in (0, 1) for first in firsts[:whole]]
    order += [(core, first) for core in (0, 1) for first in firsts[whole:]]
    return [order[n : n + per] for n in range(0, len(order), per)]


def own_kernel(split, own_ref, right_ref, normed_ref, wg_ref, out_ref, gate_ref, rights_ref):
    row_count, rows, _ = own_ref.shape
    columns = rows // row_count
    place = place_in("row", "col", "depth")
    rights = fold(k_tiles(right_ref, slice(None)), place)
    for half in range(2):
        rights_ref[half] = rights[half]
    slots = [(target, slab) for target in range(row_count) for slab in range(out_ref.shape[1])]
    units = []
    for target, slab in slots:
        first = target * columns + slab * split
        units.append(k_tiles(own_ref, slice(first, first + split)))
    for (target, slab), block in zip(slots, slab_products(split, place, rights, units)):
        out_ref[target, slab] = block
    rows, columns, channels = normed_ref.shape
    normed = normed_ref[...].reshape(rows * columns, channels)
    gate = jax.nn.sigmoid(jnp.dot(normed, wg_ref[...], preferred_element_type=jnp.float32))
    gate_ref[...] = gate.reshape(rows, columns, channels)


def other_kernel(split, slabs, done_ref, own_ref, other_ref, rights_ref, out_ref):
    row_count, rows, _ = own_ref.shape
    columns = rows // row_count
    place = place_in("row", "col", "depth")
    rights = [rights_ref[half] for half in range(2)]
    refs = (own_ref, other_ref)
    done = done_ref.shape[1]
    for start in range(0, row_count, 2):
        slots, units = [], []
        for target in (start, start + 1):
            for slab in range(done):
                out_ref[target, :, slab * LANES : (slab + 1) * LANES] = done_ref[target, slab]
            for slab in range(done, len(slabs)):
                pieces = [
                    k_tiles(refs[core], slice(target * columns + first, target * columns + first + ROWS))
                    for core, first in slabs[slab]
                ]
                slots.append((target, slab))
                units.append([jnp.concatenate(parts, axis=0) for parts in zip(*pieces)])
        for (target, slab), block in zip(slots, slab_products(split, place, rights, units)):
            out_ref[target, :, slab * LANES : (slab + 1) * LANES] = block


def output_kernel(split, slabs, sums_ref, gate_ref, gain_ref, shift_ref, w_ref, out_ref):
    columns = sums_ref.shape[1]
    channels = out_ref.shape[2]
    parity = 1 - lax.axis_index("core")

    def finish(tiles, n, js):
        normed = kernel_norm(jnp.concatenate(tiles, axis=0), gain_ref[...], shift_ref[...])
        projected = jnp.dot(normed, w_ref[...], preferred_element_type=jnp.float32)
        for piece, (core, first) in enumerate(slabs[n]):
            block, inside = divmod(first, columns)
            core = parity if core == 0 else 1 - parity
            at = pl.ds((2 * block + core) * columns + inside, ROWS)
            value = projected[piece * ROWS * ROWS : (piece + 1) * ROWS * ROWS]
            value = value.reshape(ROWS, ROWS, channels)
            out_ref[at, js, :] = (gate_ref[at, js, :] * value).astype(out_ref.dtype)

    units = [
        (n, slice(first, first + ROWS)) for n in range(len(slabs)) for first in range(0, columns, ROWS)
    ]
    for start in range(0, len(units), 2):
        both = units[start : start + 2]
        tiles = []
        for s in range(split):
            parts = [sums_ref[s, js, n * LANES : (n + 1) * LANES] for n, js in both]
            tiles.append(turn(jnp.concatenate(parts, axis=0), s))
        tiles = [turn(tile, -i) for i, tile in enumerate(spread(tiles))]
        for at, (n, js) in enumerate(both):
            finish([tile[at * ROWS : (at + 1) * ROWS] for tile in tiles], n, js)


VMEM = pl.BlockSpec(memory_space=pltpu.VMEM)
HBM = pl.BlockSpec(memory_space=pltpu.HBM)


def call(kernel, name, out_shape, specs, flops, *arrays, scratch=()):
    outs = jax.tree.leaves(out_shape)
    moved = sum(a.size * a.dtype.itemsize for a in [*arrays, *outs])
    return pl.pallas_call(
        kernel,
        name=name,
        out_shape=out_shape,
        in_specs=specs,
        out_specs=jax.tree.map(lambda _: VMEM, out_shape),
        scratch_shapes=scratch,
        cost_estimate=pl.CostEstimate(flops=flops, bytes_accessed=moved, transcendentals=0),
        compiler_params=pltpu.CompilerParams(vmem_limit_bytes=VMEM_LIMIT),
    )(*arrays)


def fast_device(pair_input, in_gain, in_shift, w_proj, w_gate, out_gain, out_shift, w_out):
    rows, columns, channels = pair_input.shape
    row_count = lax.axis_size("row")
    owners = ("row", "col", "depth")
    split = row_count * lax.axis_size("col") * lax.axis_size("depth")
    width = rows // split * LANES
    per_row = split // row_count
    slabs = pieces_of(split, columns, rows // (2 * columns))
    own_slabs = sum(all(core == 0 for core, _ in slab) for slab in slabs)
    bf16, f32 = jnp.bfloat16, jnp.float32
    shape = jax.ShapeDtypeStruct
    gains = [a.reshape(1, channels) for a in (in_gain, in_shift, out_gain, out_shift)]
    flops = 4 * rows * columns * channels * channels

    edges, normed, wg, og, os, wo = call(
        functools.partial(edges_kernel, split),
        "edges",
        (
            shape((split, 2, columns, width), bf16),
            shape(pair_input.shape, bf16),
            shape(w_gate.shape, bf16),
            shape((1, channels), f32),
            shape((1, channels), f32),
            shape(w_out.shape, bf16),
        ),
        [HBM] * 8,
        2 * flops,
        *(
            pltpu.with_memory_space_constraint(a, pltpu.HBM)
            for a in (pair_input, gains[0], gains[1], w_proj, w_gate, gains[2], gains[3], w_out)
        ),
        scratch=(
            pltpu.VMEM(pair_input.shape, bf16),
            pltpu.VMEM((1, channels), f32),
            pltpu.VMEM((1, channels), f32),
            pltpu.VMEM(w_proj.shape, bf16),
            pltpu.SemaphoreType.DMA((8,)),
        ),
    )
    exchange = functools.partial(lax.all_to_all, split_axis=0, concat_axis=0, tiled=True)
    core = lax.axis_index("core").astype(jnp.int32)
    edges, core, partner = lax.optimization_barrier((edges, core, 1 - core))
    edges = exchange(edges.reshape(2 * split, columns, width), (*owners, "core"))
    edges = edges.reshape(split, 2, columns, width)
    own, right = (
        lax.dynamic_index_in_dim(edges, at, 1, keepdims=False, allow_negative_indices=False)
        for at in (partner, core)
    )
    other = lax.ppermute(own, "core", [(0, 1), (1, 0)])
    stacked = (row_count, per_row * columns, width)
    own, other, right = (a.reshape(stacked) for a in (own, other, right))
    done, gate, rights = call(
        functools.partial(own_kernel, split),
        "own",
        (
            shape((row_count, own_slabs, per_row * columns, LANES), bf16),
            shape(pair_input.shape, f32),
            shape((2, per_row * columns, row_count * width // 2), bf16),
        ),
        [VMEM] * 4,
        flops,
        own, right, normed, wg,
    )
    sums = call(
        functools.partial(other_kernel, split, slabs),
        "other",
        shape(stacked, bf16),
        [VMEM] * 4,
        flops,
        done, own, other, rights,
    )
    sums = exchange(sums.reshape(split, columns, width), owners)
    return call(
        functools.partial(output_kernel, split, slabs),
        "output",
        shape(pair_input.shape, bf16),
        [VMEM] * 5,
        flops // 2,
        sums, gate, og, os, wo,
    )


def suits(mesh, pair_input, w_proj):
    row_count, col_count, depth_count = (mesh.shape[a] for a in ("row", "col", "depth"))
    split = row_count * col_count * depth_count // 2
    rows, columns = pair_input.shape[0] // row_count, pair_input.shape[1] // (col_count * depth_count)
    return (
        depth_count % 2 == 0
        and pair_input.shape[0] == pair_input.shape[1]
        and pair_input.shape[2] == LANES
        and w_proj.shape == (LANES, 4 * LANES)
        and split & (split - 1) == 0
        and split >= 16
        and LANES % (2 * split) == 0
        and row_count % 2 == 0
        and rows % split == 0
        and columns % ROWS == 0
        and rows % (2 * columns) == 0
    )


def solution(mesh):
    def step(pair_input, in_gain, in_shift, w_proj, w_gate, out_gain, out_shift, w_out):
        if suits(mesh, pair_input, w_proj):
            row_count, col_count, depth_count = mesh.devices.shape
            used = Mesh(
                mesh.devices.reshape(row_count, col_count, depth_count // 2, 2),
                ("row", "col", "depth", "core"),
            )
            pair, body = P("row", ("col", "depth", "core"), None), fast_device
        else:
            used, pair, body = mesh, P("row", ("col", "depth"), None), plain_device
        return jax.shard_map(
            body,
            mesh=used,
            in_specs=(pair, P(), P(), P(), P(), P(), P(), P()),
            out_specs=pair,
            check_vma=False,
        )(pair_input, in_gain, in_shift, w_proj, w_gate, out_gain, out_shift, w_out)

    return step
```

```python
import functools

import jax
import jax.numpy as jnp
from jax import lax
from jax.experimental import pallas as pl
from jax.experimental.pallas import tpu as pltpu
from jax.sharding import Mesh
from jax.sharding import PartitionSpec as P

LANES = 128
ROWS = 8
VMEM_LIMIT = 24 * 1024 * 1024
NT = (((1,), (1,)), ((), ()))


def layer_norm(values, scaling, offsets):
    average = jnp.mean(values, axis=-1, keepdims=True)
    centred = values - average
    variance = jnp.mean(centred * centred, axis=-1, keepdims=True)
    return centred * lax.rsqrt(variance + 1e-05) * scaling + offsets


def reorder_channels(values, row_count, other_count):
    shape_rest = values.shape[1:]
    grouped = values.reshape((row_count, other_count, -1) + shape_rest)
    return jnp.swapaxes(grouped, 0, 1).reshape(values.shape)


def plain_device(pair_input, in_gain, in_shift, w_proj, w_gate, out_gain, out_shift, w_out):
    row_count = lax.axis_size("row")
    others = ("col", "depth")
    other_count = lax.axis_size("col") * lax.axis_size("depth")
    channels = w_proj.shape[1] // 4
    normed = layer_norm(pair_input.astype(jnp.float32), in_gain, in_shift).astype(jnp.bfloat16)
    projected = jnp.einsum("xyc,cd->xyd", normed, w_proj, preferred_element_type=jnp.float32)
    sides = []
    for at in (0, 2 * channels):
        gate = jax.nn.sigmoid(projected[..., at : at + channels])
        side = (gate * projected[..., at + channels : at + 2 * channels]).astype(jnp.bfloat16)
        side = lax.all_to_all(side, "row", split_axis=2, concat_axis=0, tiled=True)
        sides.append(lax.all_to_all(side, others, split_axis=2, concat_axis=1, tiled=True))
    planes = jnp.einsum("kic,kjc->ijc", *sides, preferred_element_type=jnp.float32)
    product = lax.all_to_all(
        planes.astype(jnp.bfloat16), "row", split_axis=0, concat_axis=2, tiled=True
    )
    product = lax.all_to_all(product, others, split_axis=1, concat_axis=2, tiled=True)
    used = [reorder_channels(a, row_count, other_count) for a in (out_gain, out_shift, w_out)]
    product_norm = layer_norm(product.astype(jnp.float32), used[0], used[1]).astype(jnp.bfloat16)
    gating = jax.nn.sigmoid(
        jnp.einsum("xyc,cd->xyd", normed, w_gate, preferred_element_type=jnp.float32)
    )
    out = jnp.einsum("xyc,cd->xyd", product_norm, used[2], preferred_element_type=jnp.float32)
    return (gating * out).astype(jnp.bfloat16)


def spread(tiles):
    count = len(tiles)
    lane = lax.broadcasted_iota(jnp.int32, tiles[0].shape, 1)
    picked = [tiles[-v % count] for v in range(count)]
    step = 1
    while step < count:
        upper = (lane & step) != 0
        picked = [jnp.where(upper, picked[v - step], picked[v]) for v in range(count)]
        step *= 2
    return picked


def turn(tile, lanes):
    return pltpu.roll(tile, lanes % LANES, 1) if lanes % LANES else tile


def kernel_norm(values, scaling, offsets):
    share = jnp.full((LANES, LANES), 1 / LANES, jnp.bfloat16)
    centred = values.astype(jnp.float32) - jnp.dot(values, share, preferred_element_type=jnp.float32)
    variance = jnp.mean(centred * centred, axis=-1, keepdims=True)
    return (centred * lax.rsqrt(variance + 1e-05) * scaling + offsets).astype(jnp.bfloat16)


def edges_kernel(
    split, x_hbm, gain_hbm, shift_hbm, w_hbm, wg_hbm, og_hbm, os_hbm, wo_hbm,
    out_ref, normed_ref, wg_ref, og_ref, os_ref, wo_ref, x_ref, gain_ref, shift_ref, w_ref, sems,
):
    core = lax.axis_index("core")
    rows, columns, channels = x_hbm.shape
    pairs = (
        (x_hbm, x_ref), (gain_hbm, gain_ref), (shift_hbm, shift_ref), (w_hbm, w_ref),
        (wg_hbm, wg_ref), (og_hbm, og_ref), (os_hbm, os_ref), (wo_hbm, wo_ref),
    )
    copies = [pltpu.make_async_copy(a, b, sems.at[n]) for n, (a, b) in enumerate(pairs)]
    for copy in copies:
        copy.start()
    for copy in copies[:4]:
        copy.wait()
    normed = []
    for slab in range(rows // split):
        ks = slice(slab * split, (slab + 1) * split)
        values = x_ref[ks].reshape(split * columns, channels)
        normed.append(kernel_norm(values, gain_ref[...], shift_ref[...]))
        normed_ref[ks] = normed[-1].reshape(split, columns, channels)
    for slab, values in enumerate(normed):
        projected = jnp.dot(values, w_ref[...], preferred_element_type=jnp.float32)
        for i_tile in range(columns // ROWS):
            tiles = []
            for k in range(split):
                first = k * columns + i_tile * ROWS
                part = projected[first : first + ROWS]
                parts = [part[:, n * channels : (n + 1) * channels] for n in range(4)]
                left = jax.nn.sigmoid(parts[0]) * parts[1]
                right = jax.nn.sigmoid(parts[2]) * parts[3]
                both = jnp.concatenate([left, right], axis=0).astype(out_ref.dtype)
                tiles.append(turn(both, k))
            for s, tile in enumerate(spread(tiles)):
                at = slice(i_tile * ROWS, (i_tile + 1) * ROWS)
                lanes = slice(slab * LANES, (slab + 1) * LANES)
                depth_count, _, col_count, row_count = out_ref.shape[:4]
                depth, col, row = s % depth_count, s // depth_count % col_count, s // depth_count // col_count
                out_ref[depth, 1 - core, col, row, at, lanes] = tile[:ROWS]
                out_ref[depth, core, col, row, at, lanes] = tile[ROWS:]
    for copy in copies[4:]:
        copy.wait()


def place_in(*axes):
    place = lax.axis_index(axes[0])
    for axis in axes[1:]:
        place = place * lax.axis_size(axis) + lax.axis_index(axis)
    return place


def lane_place(shape, place):
    return (lax.broadcasted_iota(jnp.int32, shape, 1) - place) & (LANES - 1)


def k_tiles(ref, at):
    return [
        ref[r, at, t * LANES : (t + 1) * LANES]
        for r in range(ref.shape[0])
        for t in range(ref.shape[2] // LANES)
    ]


def fold(tiles, place):
    low = lane_place(tiles[0].shape, place) < LANES // 2
    halves = ([], [])
    for first, second in zip(tiles[::2], tiles[1::2]):
        halves[0].append(jnp.where(low, first, turn(second, LANES // 2)))
        halves[1].append(jnp.where(low, turn(first, LANES // 2), second))
    return [jnp.concatenate(half, axis=1) for half in halves]


def slab_products(split, place, rights, units):
    groups = LANES // split // 2
    shift = split.bit_length() - 1
    position = lane_place((split, LANES), place)
    group = lax.shift_right_logical(position, jnp.int32(shift)) & (groups - 1)
    count = rights[0].shape[1] // LANES
    masks = [
        jnp.concatenate([(group == g).astype(jnp.bfloat16)] * count, axis=1) for g in range(groups)
    ]
    masked = ([], [])
    for unit in units:
        for half, folded in enumerate(fold(unit, place)):
            masked[half].extend(folded * mask for mask in masks)
    low, high = (
        lax.dot_general(
            right, jnp.concatenate(parts, axis=0), NT, preferred_element_type=jnp.float32
        ).astype(jnp.bfloat16)
        for right, parts in zip(rights, masked)
    )
    first_half = lax.broadcasted_iota(jnp.int32, (rights[0].shape[0], LANES), 1) < LANES // 2
    out = []
    for n in range(0, len(units) * LANES // 2, LANES):
        lows, highs = low[:, n : n + LANES], high[:, n : n + LANES]
        out.append(jnp.where(first_half, lows, turn(highs, LANES // 2)))
        out.append(jnp.where(first_half, turn(lows, LANES // 2), highs))
    return out


def pieces_of(split, columns, row_blocks):
    firsts = list(range(0, row_blocks * columns, ROWS))
    per = split // ROWS
    whole = len(firsts) // per * per
    order = [(core, first) for core in (0, 1) for first in firsts[:whole]]
    order += [(core, first) for core in (0, 1) for first in firsts[whole:]]
    return [order[n : n + per] for n in range(0, len(order), per)]


def own_kernel(split, own_ref, right_ref, normed_ref, wg_ref, out_ref, gate_ref, rights_ref):
    row_count, rows, _ = own_ref.shape
    columns = rows // row_count
    place = place_in("row", "col", "depth")
    rights = fold(k_tiles(right_ref, slice(None)), place)
    for half in range(2):
        rights_ref[half] = rights[half]
    slots = [(target, slab) for target in range(row_count) for slab in range(out_ref.shape[1])]
    units = []
    for target, slab in slots:
        first = target * columns + slab * split
        units.append(k_tiles(own_ref, slice(first, first + split)))
    for (target, slab), block in zip(slots, slab_products(split, place, rights, units)):
        out_ref[target, slab] = block
    rows, columns, channels = normed_ref.shape
    normed = normed_ref[...].reshape(rows * columns, channels)
    gate = jax.nn.sigmoid(jnp.dot(normed, wg_ref[...], preferred_element_type=jnp.float32))
    gate_ref[...] = gate.reshape(rows, columns, channels)


def other_kernel(split, slabs, done_ref, own_ref, other_ref, rights_ref, out_ref):
    row_count, rows, _ = own_ref.shape
    columns = rows // row_count
    place = place_in("row", "col", "depth")
    rights = [rights_ref[half] for half in range(2)]
    refs = (own_ref, other_ref)
    done = done_ref.shape[1]
    for start in range(0, row_count, 2):
        slots, units = [], []
        for target in (start, start + 1):
            for slab in range(done):
                out_ref[target, :, slab * LANES : (slab + 1) * LANES] = done_ref[target, slab]
            for slab in range(done, len(slabs)):
                pieces = [
                    k_tiles(refs[core], slice(target * columns + first, target * columns + first + ROWS))
                    for core, first in slabs[slab]
                ]
                slots.append((target, slab))
                units.append([jnp.concatenate(parts, axis=0) for parts in zip(*pieces)])
        for (target, slab), block in zip(slots, slab_products(split, place, rights, units)):
            out_ref[target, :, slab * LANES : (slab + 1) * LANES] = block


def output_kernel(split, slabs, sums_ref, gate_ref, gain_ref, shift_ref, w_ref, out_ref):
    columns = sums_ref.shape[1]
    channels = out_ref.shape[2]
    parity = 1 - lax.axis_index("core")

    def finish(tiles, n, js):
        normed = kernel_norm(jnp.concatenate(tiles, axis=0), gain_ref[...], shift_ref[...])
        projected = jnp.dot(normed, w_ref[...], preferred_element_type=jnp.float32)
        for piece, (core, first) in enumerate(slabs[n]):
            block, inside = divmod(first, columns)
            core = parity if core == 0 else 1 - parity
            at = pl.ds((2 * block + core) * columns + inside, ROWS)
            value = projected[piece * ROWS * ROWS : (piece + 1) * ROWS * ROWS]
            value = value.reshape(ROWS, ROWS, channels)
            out_ref[at, js, :] = (gate_ref[at, js, :] * value).astype(out_ref.dtype)

    units = [
        (n, slice(first, first + ROWS)) for n in range(len(slabs)) for first in range(0, columns, ROWS)
    ]
    for start in range(0, len(units), 2):
        both = units[start : start + 2]
        tiles = []
        for s in range(split):
            parts = [sums_ref[s, js, n * LANES : (n + 1) * LANES] for n, js in both]
            tiles.append(turn(jnp.concatenate(parts, axis=0), s))
        tiles = [turn(tile, -i) for i, tile in enumerate(spread(tiles))]
        for at, (n, js) in enumerate(both):
            finish([tile[at * ROWS : (at + 1) * ROWS] for tile in tiles], n, js)


VMEM = pl.BlockSpec(memory_space=pltpu.VMEM)
HBM = pl.BlockSpec(memory_space=pltpu.HBM)


def call(kernel, name, out_shape, specs, flops, *arrays, scratch=()):
    outs = jax.tree.leaves(out_shape)
    moved = sum(a.size * a.dtype.itemsize for a in [*arrays, *outs])
    return pl.pallas_call(
        kernel,
        name=name,
        out_shape=out_shape,
        in_specs=specs,
        out_specs=jax.tree.map(lambda _: VMEM, out_shape),
        scratch_shapes=scratch,
        cost_estimate=pl.CostEstimate(flops=flops, bytes_accessed=moved, transcendentals=0),
        compiler_params=pltpu.CompilerParams(vmem_limit_bytes=VMEM_LIMIT),
    )(*arrays)


def fast_device(pair_input, in_gain, in_shift, w_proj, w_gate, out_gain, out_shift, w_out):
    rows, columns, channels = pair_input.shape
    row_count = lax.axis_size("row")
    owners = ("row", "col", "depth")
    col_count, depth_count = lax.axis_size("col"), lax.axis_size("depth")
    split = row_count * col_count * depth_count
    width = rows // split * LANES
    per_row = split // row_count
    slabs = pieces_of(split, columns, rows // (2 * columns))
    own_slabs = sum(all(core == 0 for core, _ in slab) for slab in slabs)
    bf16, f32 = jnp.bfloat16, jnp.float32
    shape = jax.ShapeDtypeStruct
    gains = [a.reshape(1, channels) for a in (in_gain, in_shift, out_gain, out_shift)]
    flops = 4 * rows * columns * channels * channels

    edges, normed, wg, og, os, wo = call(
        functools.partial(edges_kernel, split),
        "edges",
        (
            shape((depth_count, 2, col_count, row_count, columns, width), bf16),
            shape(pair_input.shape, bf16),
            shape(w_gate.shape, bf16),
            shape((1, channels), f32),
            shape((1, channels), f32),
            shape(w_out.shape, bf16),
        ),
        [HBM] * 8,
        2 * flops,
        *(
            pltpu.with_memory_space_constraint(a, pltpu.HBM)
            for a in (pair_input, gains[0], gains[1], w_proj, w_gate, gains[2], gains[3], w_out)
        ),
        scratch=(
            pltpu.VMEM(pair_input.shape, bf16),
            pltpu.VMEM((1, channels), f32),
            pltpu.VMEM((1, channels), f32),
            pltpu.VMEM(w_proj.shape, bf16),
            pltpu.SemaphoreType.DMA((8,)),
        ),
    )
    exchange = functools.partial(lax.all_to_all, split_axis=0, concat_axis=0, tiled=True)
    core = lax.axis_index("core").astype(jnp.int32)
    edges, core, partner = lax.optimization_barrier((edges, core, 1 - core))
    grouped = edges.shape
    edges = exchange(
        edges.reshape(2 * split, columns, width), ("depth", "core", "col", "row")
    ).reshape(grouped)
    own, right = (
        lax.dynamic_index_in_dim(edges, at, 1, keepdims=False, allow_negative_indices=False)
        .transpose(2, 1, 0, 3, 4)
        .reshape(split, columns, width)
        for at in (partner, core)
    )
    other = lax.ppermute(own, "core", [(0, 1), (1, 0)])
    stacked = (row_count, per_row * columns, width)
    own, other, right = (a.reshape(stacked) for a in (own, other, right))
    done, gate, rights = call(
        functools.partial(own_kernel, split),
        "own",
        (
            shape((row_count, own_slabs, per_row * columns, LANES), bf16),
            shape(pair_input.shape, f32),
            shape((2, per_row * columns, row_count * width // 2), bf16),
        ),
        [VMEM] * 4,
        flops,
        own, right, normed, wg,
    )
    sums = call(
        functools.partial(other_kernel, split, slabs),
        "other",
        shape(stacked, bf16),
        [VMEM] * 4,
        flops,
        done, own, other, rights,
    )
    sums = exchange(sums.reshape(split, columns, width), owners)
    return call(
        functools.partial(output_kernel, split, slabs),
        "output",
        shape(pair_input.shape, bf16),
        [VMEM] * 5,
        flops // 2,
        sums, gate, og, os, wo,
    )


def suits(mesh, pair_input, w_proj):
    row_count, col_count, depth_count = (mesh.shape[a] for a in ("row", "col", "depth"))
    split = row_count * col_count * depth_count // 2
    rows, columns = pair_input.shape[0] // row_count, pair_input.shape[1] // (col_count * depth_count)
    return (
        depth_count % 2 == 0
        and pair_input.shape[0] == pair_input.shape[1]
        and pair_input.shape[2] == LANES
        and w_proj.shape == (LANES, 4 * LANES)
        and split & (split - 1) == 0
        and split >= 16
        and LANES % (2 * split) == 0
        and row_count % 2 == 0
        and rows % split == 0
        and columns % ROWS == 0
        and rows % (2 * columns) == 0
    )


def solution(mesh):
    def step(pair_input, in_gain, in_shift, w_proj, w_gate, out_gain, out_shift, w_out):
        if suits(mesh, pair_input, w_proj):
            row_count, col_count, depth_count = mesh.devices.shape
            used = Mesh(
                mesh.devices.reshape(row_count, col_count, depth_count // 2, 2),
                ("row", "col", "depth", "core"),
            )
            pair, body = P("row", ("col", "depth", "core"), None), fast_device
        else:
            used, pair, body = mesh, P("row", ("col", "depth"), None), plain_device
        return jax.shard_map(
            body,
            mesh=used,
            in_specs=(pair, P(), P(), P(), P(), P(), P(), P()),
            out_specs=pair,
            check_vma=False,
        )(pair_input, in_gain, in_shift, w_proj, w_gate, out_gain, out_shift, w_out)

    return step
```

```python
import functools

import jax
import jax.numpy as jnp
from jax import lax
from jax.experimental import pallas as pl
from jax.experimental.pallas import tpu as pltpu
from jax.sharding import Mesh
from jax.sharding import PartitionSpec as P

LANES = 128
ROWS = 8
VMEM_LIMIT = 24 * 1024 * 1024
OWNERS = ("row_hi", "row_lo", "col", "depth")
FIRST_ORDER = ("depth", "core", "col", "row_hi", "row_lo")
LAST_ORDER = ("depth", "col", "row_lo", "row_hi")
NT = (((1,), (1,)), ((), ()))


def layer_norm(values, scaling, offsets):
    average = jnp.mean(values, axis=-1, keepdims=True)
    centred = values - average
    variance = jnp.mean(centred * centred, axis=-1, keepdims=True)
    return centred * lax.rsqrt(variance + 1e-05) * scaling + offsets


def reorder_channels(values, row_count, other_count):
    shape_rest = values.shape[1:]
    grouped = values.reshape((row_count, other_count, -1) + shape_rest)
    return jnp.swapaxes(grouped, 0, 1).reshape(values.shape)


def plain_device(pair_input, in_gain, in_shift, w_proj, w_gate, out_gain, out_shift, w_out):
    row_count = lax.axis_size("row")
    others = ("col", "depth")
    other_count = lax.axis_size("col") * lax.axis_size("depth")
    channels = w_proj.shape[1] // 4
    normed = layer_norm(pair_input.astype(jnp.float32), in_gain, in_shift).astype(jnp.bfloat16)
    projected = jnp.einsum("xyc,cd->xyd", normed, w_proj, preferred_element_type=jnp.float32)
    sides = []
    for at in (0, 2 * channels):
        gate = jax.nn.sigmoid(projected[..., at : at + channels])
        side = (gate * projected[..., at + channels : at + 2 * channels]).astype(jnp.bfloat16)
        side = lax.all_to_all(side, "row", split_axis=2, concat_axis=0, tiled=True)
        sides.append(lax.all_to_all(side, others, split_axis=2, concat_axis=1, tiled=True))
    planes = jnp.einsum("kic,kjc->ijc", *sides, preferred_element_type=jnp.float32)
    product = lax.all_to_all(
        planes.astype(jnp.bfloat16), "row", split_axis=0, concat_axis=2, tiled=True
    )
    product = lax.all_to_all(product, others, split_axis=1, concat_axis=2, tiled=True)
    used = [reorder_channels(a, row_count, other_count) for a in (out_gain, out_shift, w_out)]
    product_norm = layer_norm(product.astype(jnp.float32), used[0], used[1]).astype(jnp.bfloat16)
    gating = jax.nn.sigmoid(
        jnp.einsum("xyc,cd->xyd", normed, w_gate, preferred_element_type=jnp.float32)
    )
    out = jnp.einsum("xyc,cd->xyd", product_norm, used[2], preferred_element_type=jnp.float32)
    return (gating * out).astype(jnp.bfloat16)


def spread(tiles):
    count = len(tiles)
    lane = lax.broadcasted_iota(jnp.int32, tiles[0].shape, 1)
    picked = [tiles[-v % count] for v in range(count)]
    step = 1
    while step < count:
        upper = (lane & step) != 0
        picked = [jnp.where(upper, picked[v - step], picked[v]) for v in range(count)]
        step *= 2
    return picked


def turn(tile, lanes):
    return pltpu.roll(tile, lanes % LANES, 1) if lanes % LANES else tile


def kernel_norm(values, scaling, offsets):
    share = jnp.full((LANES, LANES), 1 / LANES, jnp.bfloat16)
    centred = values.astype(jnp.float32) - jnp.dot(values, share, preferred_element_type=jnp.float32)
    variance = jnp.mean(centred * centred, axis=-1, keepdims=True)
    return (centred * lax.rsqrt(variance + 1e-05) * scaling + offsets).astype(jnp.bfloat16)


def edges_kernel(
    split, x_hbm, gain_hbm, shift_hbm, w_hbm, wg_hbm, og_hbm, os_hbm, wo_hbm,
    out_ref, normed_ref, wg_ref, og_ref, os_ref, wo_ref, x_ref, gain_ref, shift_ref, w_ref, sems,
):
    core = lax.axis_index("core")
    rows, columns, channels = x_hbm.shape
    pairs = (
        (x_hbm, x_ref), (gain_hbm, gain_ref), (shift_hbm, shift_ref), (w_hbm, w_ref),
        (wg_hbm, wg_ref), (og_hbm, og_ref), (os_hbm, os_ref), (wo_hbm, wo_ref),
    )
    copies = [pltpu.make_async_copy(a, b, sems.at[n]) for n, (a, b) in enumerate(pairs)]
    for copy in copies:
        copy.start()
    for copy in copies[:4]:
        copy.wait()
    normed = []
    for slab in range(rows // split):
        ks = slice(slab * split, (slab + 1) * split)
        values = x_ref[ks].reshape(split * columns, channels)
        normed.append(kernel_norm(values, gain_ref[...], shift_ref[...]))
        normed_ref[ks] = normed[-1].reshape(split, columns, channels)
    for slab, values in enumerate(normed):
        projected = jnp.dot(values, w_ref[...], preferred_element_type=jnp.float32)
        for i_tile in range(columns // ROWS):
            tiles = []
            for k in range(split):
                first = k * columns + i_tile * ROWS
                part = projected[first : first + ROWS]
                parts = [part[:, n * channels : (n + 1) * channels] for n in range(4)]
                left = jax.nn.sigmoid(parts[0]) * parts[1]
                right = jax.nn.sigmoid(parts[2]) * parts[3]
                both = jnp.concatenate([left, right], axis=0).astype(out_ref.dtype)
                tiles.append(turn(both, k))
            for s, tile in enumerate(spread(tiles)):
                at = slice(i_tile * ROWS, (i_tile + 1) * ROWS)
                lanes = slice(slab * LANES, (slab + 1) * LANES)
                depth_count, _, col_count, row_count = out_ref.shape[:4]
                depth, col, row = s % depth_count, s // depth_count % col_count, s // depth_count // col_count
                out_ref[depth, 1 - core, col, row, at, lanes] = tile[:ROWS]
                out_ref[depth, core, col, row, at, lanes] = tile[ROWS:]
    for copy in copies[4:]:
        copy.wait()


def place_in(*axes):
    place = lax.axis_index(axes[0])
    for axis in axes[1:]:
        place = place * lax.axis_size(axis) + lax.axis_index(axis)
    return place


def lane_place(shape, place):
    return (lax.broadcasted_iota(jnp.int32, shape, 1) - place) & (LANES - 1)


def k_tiles(ref, at):
    return [
        ref[r, at, t * LANES : (t + 1) * LANES]
        for r in range(ref.shape[0])
        for t in range(ref.shape[2] // LANES)
    ]


def fold(tiles, place):
    low = lane_place(tiles[0].shape, place) < LANES // 2
    halves = ([], [])
    for first, second in zip(tiles[::2], tiles[1::2]):
        halves[0].append(jnp.where(low, first, turn(second, LANES // 2)))
        halves[1].append(jnp.where(low, turn(first, LANES // 2), second))
    return [jnp.concatenate(half, axis=1) for half in halves]


def slab_products(split, place, rights, units):
    groups = LANES // split // 2
    shift = split.bit_length() - 1
    position = lane_place((split, LANES), place)
    group = lax.shift_right_logical(position, jnp.int32(shift)) & (groups - 1)
    count = rights[0].shape[1] // LANES
    masks = [
        jnp.concatenate([(group == g).astype(jnp.bfloat16)] * count, axis=1) for g in range(groups)
    ]
    masked = ([], [])
    for unit in units:
        for half, folded in enumerate(fold(unit, place)):
            masked[half].extend(folded * mask for mask in masks)
    low, high = (
        lax.dot_general(
            right, jnp.concatenate(parts, axis=0), NT, preferred_element_type=jnp.float32
        ).astype(jnp.bfloat16)
        for right, parts in zip(rights, masked)
    )
    first_half = lax.broadcasted_iota(jnp.int32, (rights[0].shape[0], LANES), 1) < LANES // 2
    out = []
    for n in range(0, len(units) * LANES // 2, LANES):
        lows, highs = low[:, n : n + LANES], high[:, n : n + LANES]
        out.append(jnp.where(first_half, lows, turn(highs, LANES // 2)))
        out.append(jnp.where(first_half, turn(lows, LANES // 2), highs))
    return out


def pieces_of(split, columns, row_blocks):
    firsts = list(range(0, row_blocks * columns, ROWS))
    per = split // ROWS
    whole = len(firsts) // per * per
    order = [(core, first) for core in (0, 1) for first in firsts[:whole]]
    order += [(core, first) for core in (0, 1) for first in firsts[whole:]]
    return [order[n : n + per] for n in range(0, len(order), per)]


def own_kernel(split, own_ref, right_ref, normed_ref, wg_ref, out_ref, gate_ref, rights_ref):
    row_count, rows, _ = own_ref.shape
    columns = rows // row_count
    place = place_in(*OWNERS)
    rights = fold(k_tiles(right_ref, slice(None)), place)
    for half in range(2):
        rights_ref[half] = rights[half]
    slots = [(target, slab) for target in range(row_count) for slab in range(out_ref.shape[1])]
    units = []
    for target, slab in slots:
        first = target * columns + slab * split
        units.append(k_tiles(own_ref, slice(first, first + split)))
    for (target, slab), block in zip(slots, slab_products(split, place, rights, units)):
        out_ref[target, slab] = block
    rows, columns, channels = normed_ref.shape
    normed = normed_ref[...].reshape(rows * columns, channels)
    gate = jax.nn.sigmoid(jnp.dot(normed, wg_ref[...], preferred_element_type=jnp.float32))
    gate_ref[...] = gate.reshape(rows, columns, channels)


def other_kernel(split, slabs, done_ref, own_ref, other_ref, rights_ref, out_ref):
    row_count, rows, _ = own_ref.shape
    columns = rows // row_count
    place = place_in(*OWNERS)
    rights = [rights_ref[half] for half in range(2)]
    refs = (own_ref, other_ref)
    done = done_ref.shape[1]
    for start in range(0, row_count, 2):
        slots, units = [], []
        for target in (start, start + 1):
            for slab in range(done):
                out_ref[target, :, slab * LANES : (slab + 1) * LANES] = done_ref[target, slab]
            for slab in range(done, len(slabs)):
                pieces = [
                    k_tiles(refs[core], slice(target * columns + first, target * columns + first + ROWS))
                    for core, first in slabs[slab]
                ]
                slots.append((target, slab))
                units.append([jnp.concatenate(parts, axis=0) for parts in zip(*pieces)])
        for (target, slab), block in zip(slots, slab_products(split, place, rights, units)):
            out_ref[target, :, slab * LANES : (slab + 1) * LANES] = block


def output_kernel(split, slabs, sums_ref, gate_ref, gain_ref, shift_ref, w_ref, out_ref):
    depth_count, col_count, low_count, _, columns, _ = sums_ref.shape
    channels = out_ref.shape[2]
    parity = 1 - lax.axis_index("core")

    def finish(tiles, n, js):
        normed = kernel_norm(jnp.concatenate(tiles, axis=0), gain_ref[...], shift_ref[...])
        projected = jnp.dot(normed, w_ref[...], preferred_element_type=jnp.float32)
        for piece, (core, first) in enumerate(slabs[n]):
            block, inside = divmod(first, columns)
            core = parity if core == 0 else 1 - parity
            at = pl.ds((2 * block + core) * columns + inside, ROWS)
            value = projected[piece * ROWS * ROWS : (piece + 1) * ROWS * ROWS]
            value = value.reshape(ROWS, ROWS, channels)
            out_ref[at, js, :] = (gate_ref[at, js, :] * value).astype(out_ref.dtype)

    units = [
        (n, slice(first, first + ROWS)) for n in range(len(slabs)) for first in range(0, columns, ROWS)
    ]
    for start in range(0, len(units), 2):
        both = units[start : start + 2]
        tiles = []
        for s in range(split):
            rest, depth = divmod(s, depth_count)
            rest, col = divmod(rest, col_count)
            high, low = divmod(rest, low_count)
            parts = [
                sums_ref[depth, col, low, high, js, n * LANES : (n + 1) * LANES] for n, js in both
            ]
            tiles.append(turn(jnp.concatenate(parts, axis=0), s))
        tiles = [turn(tile, -i) for i, tile in enumerate(spread(tiles))]
        for at, (n, js) in enumerate(both):
            finish([tile[at * ROWS : (at + 1) * ROWS] for tile in tiles], n, js)


VMEM = pl.BlockSpec(memory_space=pltpu.VMEM)
HBM = pl.BlockSpec(memory_space=pltpu.HBM)


def call(kernel, name, out_shape, specs, flops, *arrays, scratch=()):
    outs = jax.tree.leaves(out_shape)
    moved = sum(a.size * a.dtype.itemsize for a in [*arrays, *outs])
    return pl.pallas_call(
        kernel,
        name=name,
        out_shape=out_shape,
        in_specs=specs,
        out_specs=jax.tree.map(lambda _: VMEM, out_shape),
        scratch_shapes=scratch,
        cost_estimate=pl.CostEstimate(flops=flops, bytes_accessed=moved, transcendentals=0),
        compiler_params=pltpu.CompilerParams(vmem_limit_bytes=VMEM_LIMIT),
    )(*arrays)


def fast_device(pair_input, in_gain, in_shift, w_proj, w_gate, out_gain, out_shift, w_out):
    rows, columns, channels = pair_input.shape
    high_count, low_count, col_count, depth_count = (lax.axis_size(axis) for axis in OWNERS)
    row_count = high_count * low_count
    split = row_count * col_count * depth_count
    width = rows // split * LANES
    per_row = split // row_count
    slabs = pieces_of(split, columns, rows // (2 * columns))
    own_slabs = sum(all(core == 0 for core, _ in slab) for slab in slabs)
    bf16, f32 = jnp.bfloat16, jnp.float32
    shape = jax.ShapeDtypeStruct
    gains = [a.reshape(1, channels) for a in (in_gain, in_shift, out_gain, out_shift)]
    flops = 4 * rows * columns * channels * channels

    edges, normed, wg, og, os, wo = call(
        functools.partial(edges_kernel, split),
        "edges",
        (
            shape((depth_count, 2, col_count, row_count, columns, width), bf16),
            shape(pair_input.shape, bf16),
            shape(w_gate.shape, bf16),
            shape((1, channels), f32),
            shape((1, channels), f32),
            shape(w_out.shape, bf16),
        ),
        [HBM] * 8,
        2 * flops,
        *(
            pltpu.with_memory_space_constraint(a, pltpu.HBM)
            for a in (pair_input, gains[0], gains[1], w_proj, w_gate, gains[2], gains[3], w_out)
        ),
        scratch=(
            pltpu.VMEM(pair_input.shape, bf16),
            pltpu.VMEM((1, channels), f32),
            pltpu.VMEM((1, channels), f32),
            pltpu.VMEM(w_proj.shape, bf16),
            pltpu.SemaphoreType.DMA((8,)),
        ),
    )
    exchange = functools.partial(lax.all_to_all, split_axis=0, concat_axis=0, tiled=True)
    core = lax.axis_index("core").astype(jnp.int32)
    edges, core, partner = lax.optimization_barrier((edges, core, 1 - core))
    grouped = edges.shape
    edges = exchange(
        edges.reshape(2 * split, columns, width), FIRST_ORDER
    ).reshape(grouped)
    own, right = (
        lax.dynamic_index_in_dim(edges, at, 1, keepdims=False, allow_negative_indices=False)
        .transpose(2, 1, 0, 3, 4)
        .reshape(split, columns, width)
        for at in (partner, core)
    )
    other = lax.ppermute(own, "core", [(0, 1), (1, 0)])
    stacked = (row_count, per_row * columns, width)
    own, other, right = (a.reshape(stacked) for a in (own, other, right))
    done, gate, rights = call(
        functools.partial(own_kernel, split),
        "own",
        (
            shape((row_count, own_slabs, per_row * columns, LANES), bf16),
            shape(pair_input.shape, f32),
            shape((2, per_row * columns, row_count * width // 2), bf16),
        ),
        [VMEM] * 4,
        flops,
        own, right, normed, wg,
    )
    sums = call(
        functools.partial(other_kernel, split, slabs),
        "other",
        shape(stacked, bf16),
        [VMEM] * 4,
        flops,
        done, own, other, rights,
    )
    sums = sums.reshape(high_count, low_count, col_count, depth_count, columns, width)
    sums = sums.transpose(3, 2, 1, 0, 4, 5)
    grouped = sums.shape
    sums = exchange(sums.reshape(split, columns, width), LAST_ORDER).reshape(grouped)
    return call(
        functools.partial(output_kernel, split, slabs),
        "output",
        shape(pair_input.shape, bf16),
        [VMEM] * 5,
        flops // 2,
        sums, gate, og, os, wo,
    )


def suits(mesh, pair_input, w_proj):
    row_count, col_count, depth_count = (mesh.shape[a] for a in ("row", "col", "depth"))
    split = row_count * col_count * depth_count // 2
    rows, columns = pair_input.shape[0] // row_count, pair_input.shape[1] // (col_count * depth_count)
    return (
        depth_count % 2 == 0
        and pair_input.shape[0] == pair_input.shape[1]
        and pair_input.shape[2] == LANES
        and w_proj.shape == (LANES, 4 * LANES)
        and split & (split - 1) == 0
        and split >= 16
        and LANES % (2 * split) == 0
        and row_count % 2 == 0
        and rows % split == 0
        and columns % ROWS == 0
        and rows % (2 * columns) == 0
    )


def solution(mesh):
    def step(pair_input, in_gain, in_shift, w_proj, w_gate, out_gain, out_shift, w_out):
        if suits(mesh, pair_input, w_proj):
            row_count, col_count, depth_count = mesh.devices.shape
            used = Mesh(
                mesh.devices.reshape(row_count // 2, 2, col_count, depth_count // 2, 2),
                (*OWNERS, "core"),
            )
            pair = P(("row_hi", "row_lo"), ("col", "depth", "core"), None)
            body = fast_device
        else:
            used, pair, body = mesh, P("row", ("col", "depth"), None), plain_device
        return jax.shard_map(
            body,
            mesh=used,
            in_specs=(pair, P(), P(), P(), P(), P(), P(), P()),
            out_specs=pair,
            check_vma=False,
        )(pair_input, in_gain, in_shift, w_proj, w_gate, out_gain, out_shift, w_out)

    return step
```

```python
import functools

import jax
import jax.numpy as jnp
from jax import lax
from jax.experimental import pallas as pl
from jax.experimental.pallas import tpu as pltpu
from jax.sharding import Mesh
from jax.sharding import PartitionSpec as P

LANES = 128
ROWS = 8
VMEM_LIMIT = 24 * 1024 * 1024
OWNERS = ("row_hi", "row_lo", "col", "depth")
FIRST_ORDER = ("depth", "core", "col", "row_hi", "row_lo")
LAST_ORDER = ("depth", "col", "row_lo", "row_hi")
NT = (((1,), (1,)), ((), ()))


def layer_norm(values, scaling, offsets):
    average = jnp.mean(values, axis=-1, keepdims=True)
    centred = values - average
    variance = jnp.mean(centred * centred, axis=-1, keepdims=True)
    return centred * lax.rsqrt(variance + 1e-05) * scaling + offsets


def reorder_channels(values, row_count, other_count):
    shape_rest = values.shape[1:]
    grouped = values.reshape((row_count, other_count, -1) + shape_rest)
    return jnp.swapaxes(grouped, 0, 1).reshape(values.shape)


def plain_device(pair_input, in_gain, in_shift, w_proj, w_gate, out_gain, out_shift, w_out):
    row_count = lax.axis_size("row")
    others = ("col", "depth")
    other_count = lax.axis_size("col") * lax.axis_size("depth")
    channels = w_proj.shape[1] // 4
    normed = layer_norm(pair_input.astype(jnp.float32), in_gain, in_shift).astype(jnp.bfloat16)
    projected = jnp.einsum("xyc,cd->xyd", normed, w_proj, preferred_element_type=jnp.float32)
    sides = []
    for at in (0, 2 * channels):
        gate = jax.nn.sigmoid(projected[..., at : at + channels])
        side = (gate * projected[..., at + channels : at + 2 * channels]).astype(jnp.bfloat16)
        side = lax.all_to_all(side, "row", split_axis=2, concat_axis=0, tiled=True)
        sides.append(lax.all_to_all(side, others, split_axis=2, concat_axis=1, tiled=True))
    planes = jnp.einsum("kic,kjc->ijc", *sides, preferred_element_type=jnp.float32)
    product = lax.all_to_all(
        planes.astype(jnp.bfloat16), "row", split_axis=0, concat_axis=2, tiled=True
    )
    product = lax.all_to_all(product, others, split_axis=1, concat_axis=2, tiled=True)
    used = [reorder_channels(a, row_count, other_count) for a in (out_gain, out_shift, w_out)]
    product_norm = layer_norm(product.astype(jnp.float32), used[0], used[1]).astype(jnp.bfloat16)
    gating = jax.nn.sigmoid(
        jnp.einsum("xyc,cd->xyd", normed, w_gate, preferred_element_type=jnp.float32)
    )
    out = jnp.einsum("xyc,cd->xyd", product_norm, used[2], preferred_element_type=jnp.float32)
    return (gating * out).astype(jnp.bfloat16)


def spread(tiles):
    count = len(tiles)
    lane = lax.broadcasted_iota(jnp.int32, tiles[0].shape, 1)
    picked = [tiles[-v % count] for v in range(count)]
    step = 1
    while step < count:
        upper = (lane & step) != 0
        picked = [jnp.where(upper, picked[v - step], picked[v]) for v in range(count)]
        step *= 2
    return picked


def turn(tile, lanes):
    return pltpu.roll(tile, lanes % LANES, 1) if lanes % LANES else tile


def kernel_norm(values, scaling, offsets):
    share = jnp.full((LANES, LANES), 1 / LANES, jnp.bfloat16)
    centred = values.astype(jnp.float32) - jnp.dot(values, share, preferred_element_type=jnp.float32)
    variance = jnp.mean(centred * centred, axis=-1, keepdims=True)
    return (centred * lax.rsqrt(variance + 1e-05) * scaling + offsets).astype(jnp.bfloat16)


def edges_kernel(
    split, x_hbm, gain_hbm, shift_hbm, w_hbm, wg_hbm, og_hbm, os_hbm, wo_hbm,
    out_ref, normed_ref, wg_ref, og_ref, os_ref, wo_ref, x_ref, gain_ref, shift_ref, w_ref, sems,
):
    core = lax.axis_index("core")
    rows, columns, channels = x_hbm.shape
    pairs = (
        (x_hbm, x_ref), (gain_hbm, gain_ref), (shift_hbm, shift_ref), (w_hbm, w_ref),
        (wg_hbm, wg_ref), (og_hbm, og_ref), (os_hbm, os_ref), (wo_hbm, wo_ref),
    )
    copies = [pltpu.make_async_copy(a, b, sems.at[n]) for n, (a, b) in enumerate(pairs)]
    for copy in copies:
        copy.start()
    for copy in copies[:4]:
        copy.wait()
    normed = []
    for slab in range(rows // split):
        ks = slice(slab * split, (slab + 1) * split)
        values = x_ref[ks].reshape(split * columns, channels)
        normed.append(kernel_norm(values, gain_ref[...], shift_ref[...]))
        normed_ref[ks] = normed[-1].reshape(split, columns, channels)
    for slab, values in enumerate(normed):
        projected = jnp.dot(values, w_ref[...], preferred_element_type=jnp.float32)
        for i_tile in range(columns // ROWS):
            tiles = []
            for k in range(split):
                first = k * columns + i_tile * ROWS
                part = projected[first : first + ROWS]
                parts = [part[:, n * channels : (n + 1) * channels] for n in range(4)]
                left = jax.nn.sigmoid(parts[0]) * parts[1]
                right = jax.nn.sigmoid(parts[2]) * parts[3]
                both = jnp.concatenate([left, right], axis=0).astype(out_ref.dtype)
                tiles.append(turn(both, k))
            for s, tile in enumerate(spread(tiles)):
                at = slice(i_tile * ROWS, (i_tile + 1) * ROWS)
                lanes = slice(slab * LANES, (slab + 1) * LANES)
                depth_count, _, col_count, row_count = out_ref.shape[:4]
                depth, col, row = s % depth_count, s // depth_count % col_count, s // depth_count // col_count
                out_ref[depth, 1 - core, col, row, at, lanes] = tile[:ROWS]
                out_ref[depth, core, col, row, at, lanes] = tile[ROWS:]
    for copy in copies[4:]:
        copy.wait()


def place_in(*axes):
    place = lax.axis_index(axes[0])
    for axis in axes[1:]:
        place = place * lax.axis_size(axis) + lax.axis_index(axis)
    return place


def lane_place(shape, place):
    return (lax.broadcasted_iota(jnp.int32, shape, 1) - place) & (LANES - 1)


def k_tiles(ref, at):
    return [
        ref[r, at, t * LANES : (t + 1) * LANES]
        for r in range(ref.shape[0])
        for t in range(ref.shape[2] // LANES)
    ]


def fold(tiles, place):
    low = lane_place(tiles[0].shape, place) < LANES // 2
    halves = ([], [])
    for first, second in zip(tiles[::2], tiles[1::2]):
        halves[0].append(jnp.where(low, first, turn(second, LANES // 2)))
        halves[1].append(jnp.where(low, turn(first, LANES // 2), second))
    return [jnp.concatenate(half, axis=1) for half in halves]


def slab_products(split, place, rights, units):
    groups = LANES // split // 2
    shift = split.bit_length() - 1
    position = lane_place((split, LANES), place)
    group = lax.shift_right_logical(position, jnp.int32(shift)) & (groups - 1)
    count = rights[0].shape[1] // LANES
    masks = [
        jnp.concatenate([(group == g).astype(jnp.bfloat16)] * count, axis=1) for g in range(groups)
    ]
    masked = ([], [])
    for unit in units:
        for half, folded in enumerate(fold(unit, place)):
            masked[half].extend(folded * mask for mask in masks)
    low, high = (
        lax.dot_general(
            right, jnp.concatenate(parts, axis=0), NT, preferred_element_type=jnp.float32
        ).astype(jnp.bfloat16)
        for right, parts in zip(rights, masked)
    )
    first_half = lax.broadcasted_iota(jnp.int32, (rights[0].shape[0], LANES), 1) < LANES // 2
    out = []
    for n in range(0, len(units) * LANES // 2, LANES):
        lows, highs = low[:, n : n + LANES], high[:, n : n + LANES]
        out.append(jnp.where(first_half, lows, turn(highs, LANES // 2)))
        out.append(jnp.where(first_half, turn(lows, LANES // 2), highs))
    return out


def pieces_of(split, columns, row_blocks):
    firsts = list(range(0, row_blocks * columns, ROWS))
    per = split // ROWS
    whole = len(firsts) // per * per
    order = [(core, first) for core in (0, 1) for first in firsts[:whole]]
    order += [(core, first) for core in (0, 1) for first in firsts[whole:]]
    return [order[n : n + per] for n in range(0, len(order), per)]


def own_kernel(split, own_ref, right_ref, normed_ref, wg_ref, out_ref, gate_ref, rights_ref):
    row_count, rows, _ = own_ref.shape
    columns = rows // row_count
    place = place_in(*OWNERS)
    rights = fold(k_tiles(right_ref, slice(None)), place)
    for half in range(2):
        rights_ref[half] = rights[half]
    slots = [(target, slab) for target in range(row_count) for slab in range(out_ref.shape[1])]
    units = []
    for target, slab in slots:
        first = target * columns + slab * split
        units.append(k_tiles(own_ref, slice(first, first + split)))
    for (target, slab), block in zip(slots, slab_products(split, place, rights, units)):
        out_ref[target, slab] = block
    rows, columns, channels = normed_ref.shape
    normed = normed_ref[...].reshape(rows * columns, channels)
    gate = jax.nn.sigmoid(jnp.dot(normed, wg_ref[...], preferred_element_type=jnp.float32))
    gate_ref[...] = gate.reshape(rows, columns, channels)


def other_kernel(split, slabs, done_ref, own_ref, other_ref, rights_ref, out_ref):
    row_count, rows, _ = own_ref.shape
    columns = rows // row_count
    place = place_in(*OWNERS)
    rights = [rights_ref[half] for half in range(2)]
    refs = (own_ref, other_ref)
    done = done_ref.shape[1]
    for start in range(0, row_count, 2):
        slots, units = [], []
        for target in (start, start + 1):
            for slab in range(done):
                out_ref[target, :, slab * LANES : (slab + 1) * LANES] = done_ref[target, slab]
            for slab in range(done, len(slabs)):
                pieces = [
                    k_tiles(refs[core], slice(target * columns + first, target * columns + first + ROWS))
                    for core, first in slabs[slab]
                ]
                slots.append((target, slab))
                units.append([jnp.concatenate(parts, axis=0) for parts in zip(*pieces)])
        for (target, slab), block in zip(slots, slab_products(split, place, rights, units)):
            out_ref[target, :, slab * LANES : (slab + 1) * LANES] = block


def output_kernel(split, slabs, sums_ref, gate_ref, gain_ref, shift_ref, w_ref, out_ref):
    depth_count, col_count, low_count, _, columns, _ = sums_ref.shape
    channels = out_ref.shape[2]
    parity = 1 - lax.axis_index("core")

    def finish(tiles, n, js):
        normed = kernel_norm(jnp.concatenate(tiles, axis=0), gain_ref[...], shift_ref[...])
        projected = jnp.dot(normed, w_ref[...], preferred_element_type=jnp.float32)
        for piece, (core, first) in enumerate(slabs[n]):
            block, inside = divmod(first, columns)
            core = parity if core == 0 else 1 - parity
            at = pl.ds((2 * block + core) * columns + inside, ROWS)
            value = projected[piece * ROWS * ROWS : (piece + 1) * ROWS * ROWS]
            value = value.reshape(ROWS, ROWS, channels)
            out_ref[at, js, :] = (gate_ref[at, js, :] * value).astype(out_ref.dtype)

    units = [
        (n, slice(first, first + ROWS)) for n in range(len(slabs)) for first in range(0, columns, ROWS)
    ]
    for start in range(0, len(units), 2):
        both = units[start : start + 2]
        tiles = []
        for s in range(split):
            rest, depth = divmod(s, depth_count)
            rest, col = divmod(rest, col_count)
            high, low = divmod(rest, low_count)
            parts = [
                sums_ref[depth, col, low, high, js, n * LANES : (n + 1) * LANES] for n, js in both
            ]
            tiles.append(turn(jnp.concatenate(parts, axis=0), s))
        tiles = [turn(tile, -i) for i, tile in enumerate(spread(tiles))]
        for at, (n, js) in enumerate(both):
            finish([tile[at * ROWS : (at + 1) * ROWS] for tile in tiles], n, js)


VMEM = pl.BlockSpec(memory_space=pltpu.VMEM)
HBM = pl.BlockSpec(memory_space=pltpu.HBM)


def call(kernel, name, out_shape, specs, flops, *arrays, scratch=()):
    outs = jax.tree.leaves(out_shape)
    moved = sum(a.size * a.dtype.itemsize for a in [*arrays, *outs])
    return pl.pallas_call(
        kernel,
        name=name,
        out_shape=out_shape,
        in_specs=specs,
        out_specs=jax.tree.map(lambda _: VMEM, out_shape),
        scratch_shapes=scratch,
        cost_estimate=pl.CostEstimate(flops=flops, bytes_accessed=moved, transcendentals=0),
        compiler_params=pltpu.CompilerParams(vmem_limit_bytes=VMEM_LIMIT),
    )(*arrays)


def fast_device(pair_input, in_gain, in_shift, w_proj, w_gate, out_gain, out_shift, w_out):
    rows, columns, channels = pair_input.shape
    high_count, low_count, col_count, depth_count = (lax.axis_size(axis) for axis in OWNERS)
    row_count = high_count * low_count
    split = row_count * col_count * depth_count
    width = rows // split * LANES
    per_row = split // row_count
    slabs = pieces_of(split, columns, rows // (2 * columns))
    own_slabs = sum(all(core == 0 for core, _ in slab) for slab in slabs)
    bf16, f32 = jnp.bfloat16, jnp.float32
    shape = jax.ShapeDtypeStruct
    gains = [a.reshape(1, channels) for a in (in_gain, in_shift, out_gain, out_shift)]
    flops = 4 * rows * columns * channels * channels

    edges, normed, wg, og, os, wo = call(
        functools.partial(edges_kernel, split),
        "edges",
        (
            shape((depth_count, 2, col_count, row_count, columns, width), bf16),
            shape(pair_input.shape, bf16),
            shape(w_gate.shape, bf16),
            shape((1, channels), f32),
            shape((1, channels), f32),
            shape(w_out.shape, bf16),
        ),
        [HBM] * 8,
        2 * flops,
        *(
            pltpu.with_memory_space_constraint(a, pltpu.HBM)
            for a in (pair_input, gains[0], gains[1], w_proj, w_gate, gains[2], gains[3], w_out)
        ),
        scratch=(
            pltpu.VMEM(pair_input.shape, bf16),
            pltpu.VMEM((1, channels), f32),
            pltpu.VMEM((1, channels), f32),
            pltpu.VMEM(w_proj.shape, bf16),
            pltpu.SemaphoreType.DMA((8,)),
        ),
    )
    exchange = functools.partial(lax.all_to_all, split_axis=0, concat_axis=0, tiled=True)
    core = lax.axis_index("core").astype(jnp.int32)
    edges, core, partner = lax.optimization_barrier((edges, core, 1 - core))
    grouped = edges.shape
    edges = exchange(
        edges.reshape(2 * split, columns, width), FIRST_ORDER
    ).reshape(grouped)
    def side(array, at):
        piece = lax.dynamic_index_in_dim(array, at, 1, keepdims=False, allow_negative_indices=False)
        return piece.transpose(2, 1, 0, 3, 4).reshape(split, columns, width)

    own, edges = lax.optimization_barrier((side(edges, partner), edges))
    right = side(edges, core)
    other = lax.ppermute(own, "core", [(0, 1), (1, 0)])
    stacked = (row_count, per_row * columns, width)
    own, other, right = (a.reshape(stacked) for a in (own, other, right))
    done, gate, rights = call(
        functools.partial(own_kernel, split),
        "own",
        (
            shape((row_count, own_slabs, per_row * columns, LANES), bf16),
            shape(pair_input.shape, f32),
            shape((2, per_row * columns, row_count * width // 2), bf16),
        ),
        [VMEM] * 4,
        flops,
        own, right, normed, wg,
    )
    sums = call(
        functools.partial(other_kernel, split, slabs),
        "other",
        shape(stacked, bf16),
        [VMEM] * 4,
        flops,
        done, own, other, rights,
    )
    sums = sums.reshape(high_count, low_count, col_count, depth_count, columns, width)
    sums = sums.transpose(3, 2, 1, 0, 4, 5)
    grouped = sums.shape
    sums = exchange(sums.reshape(split, columns, width), LAST_ORDER).reshape(grouped)
    return call(
        functools.partial(output_kernel, split, slabs),
        "output",
        shape(pair_input.shape, bf16),
        [VMEM] * 5,
        flops // 2,
        sums, gate, og, os, wo,
    )


def suits(mesh, pair_input, w_proj):
    row_count, col_count, depth_count = (mesh.shape[a] for a in ("row", "col", "depth"))
    split = row_count * col_count * depth_count // 2
    rows, columns = pair_input.shape[0] // row_count, pair_input.shape[1] // (col_count * depth_count)
    return (
        depth_count % 2 == 0
        and pair_input.shape[0] == pair_input.shape[1]
        and pair_input.shape[2] == LANES
        and w_proj.shape == (LANES, 4 * LANES)
        and split & (split - 1) == 0
        and split >= 16
        and LANES % (2 * split) == 0
        and row_count % 2 == 0
        and rows % split == 0
        and columns % ROWS == 0
        and rows % (2 * columns) == 0
    )


def solution(mesh):
    def step(pair_input, in_gain, in_shift, w_proj, w_gate, out_gain, out_shift, w_out):
        if suits(mesh, pair_input, w_proj):
            row_count, col_count, depth_count = mesh.devices.shape
            used = Mesh(
                mesh.devices.reshape(row_count // 2, 2, col_count, depth_count // 2, 2),
                (*OWNERS, "core"),
            )
            pair = P(("row_hi", "row_lo"), ("col", "depth", "core"), None)
            body = fast_device
        else:
            used, pair, body = mesh, P("row", ("col", "depth"), None), plain_device
        return jax.shard_map(
            body,
            mesh=used,
            in_specs=(pair, P(), P(), P(), P(), P(), P(), P()),
            out_specs=pair,
            check_vma=False,
        )(pair_input, in_gain, in_shift, w_proj, w_gate, out_gain, out_shift, w_out)

    return step
```

```python
import functools

import jax
import jax.numpy as jnp
from jax import lax
from jax.experimental import pallas as pl
from jax.experimental.pallas import tpu as pltpu
from jax.sharding import Mesh
from jax.sharding import PartitionSpec as P

LANES = 128
ROWS = 8
VMEM_LIMIT = 24 * 1024 * 1024
OWNERS = ("row_hi", "row_lo", "col", "depth")
FIRST_ORDER = ("depth", "core", "col", "row_hi", "row_lo")
LAST_ORDER = ("depth", "col", "row_lo", "row_hi")
NT = (((1,), (1,)), ((), ()))


def layer_norm(values, scaling, offsets):
    average = jnp.mean(values, axis=-1, keepdims=True)
    centred = values - average
    variance = jnp.mean(centred * centred, axis=-1, keepdims=True)
    return centred * lax.rsqrt(variance + 1e-05) * scaling + offsets


def reorder_channels(values, row_count, other_count):
    shape_rest = values.shape[1:]
    grouped = values.reshape((row_count, other_count, -1) + shape_rest)
    return jnp.swapaxes(grouped, 0, 1).reshape(values.shape)


def plain_device(pair_input, in_gain, in_shift, w_proj, w_gate, out_gain, out_shift, w_out):
    row_count = lax.axis_size("row")
    others = ("col", "depth")
    other_count = lax.axis_size("col") * lax.axis_size("depth")
    channels = w_proj.shape[1] // 4
    normed = layer_norm(pair_input.astype(jnp.float32), in_gain, in_shift).astype(jnp.bfloat16)
    projected = jnp.einsum("xyc,cd->xyd", normed, w_proj, preferred_element_type=jnp.float32)
    sides = []
    for at in (0, 2 * channels):
        gate = jax.nn.sigmoid(projected[..., at : at + channels])
        side = (gate * projected[..., at + channels : at + 2 * channels]).astype(jnp.bfloat16)
        side = lax.all_to_all(side, "row", split_axis=2, concat_axis=0, tiled=True)
        sides.append(lax.all_to_all(side, others, split_axis=2, concat_axis=1, tiled=True))
    planes = jnp.einsum("kic,kjc->ijc", *sides, preferred_element_type=jnp.float32)
    product = lax.all_to_all(
        planes.astype(jnp.bfloat16), "row", split_axis=0, concat_axis=2, tiled=True
    )
    product = lax.all_to_all(product, others, split_axis=1, concat_axis=2, tiled=True)
    used = [reorder_channels(a, row_count, other_count) for a in (out_gain, out_shift, w_out)]
    product_norm = layer_norm(product.astype(jnp.float32), used[0], used[1]).astype(jnp.bfloat16)
    gating = jax.nn.sigmoid(
        jnp.einsum("xyc,cd->xyd", normed, w_gate, preferred_element_type=jnp.float32)
    )
    out = jnp.einsum("xyc,cd->xyd", product_norm, used[2], preferred_element_type=jnp.float32)
    return (gating * out).astype(jnp.bfloat16)


def spread(tiles):
    count = len(tiles)
    lane = lax.broadcasted_iota(jnp.int32, tiles[0].shape, 1)
    picked = [tiles[-v % count] for v in range(count)]
    step = 1
    while step < count:
        upper = (lane & step) != 0
        picked = [jnp.where(upper, picked[v - step], picked[v]) for v in range(count)]
        step *= 2
    return picked


def turn(tile, lanes):
    return pltpu.roll(tile, lanes % LANES, 1) if lanes % LANES else tile


def kernel_norm(values, scaling, offsets):
    share = jnp.full((LANES, LANES), 1 / LANES, jnp.bfloat16)
    centred = values.astype(jnp.float32) - jnp.dot(values, share, preferred_element_type=jnp.float32)
    variance = jnp.mean(centred * centred, axis=-1, keepdims=True)
    return (centred * lax.rsqrt(variance + 1e-05) * scaling + offsets).astype(jnp.bfloat16)


def edges_kernel(
    split, x_hbm, gain_hbm, shift_hbm, w_hbm, wg_hbm, og_hbm, os_hbm, wo_hbm,
    out_ref, normed_ref, wg_ref, og_ref, os_ref, wo_ref, x_ref, gain_ref, shift_ref, w_ref, sems,
):
    core = lax.axis_index("core")
    rows, columns, channels = x_hbm.shape
    pairs = (
        (x_hbm, x_ref), (gain_hbm, gain_ref), (shift_hbm, shift_ref), (w_hbm, w_ref),
        (wg_hbm, wg_ref), (og_hbm, og_ref), (os_hbm, os_ref), (wo_hbm, wo_ref),
    )
    copies = [pltpu.make_async_copy(a, b, sems.at[n]) for n, (a, b) in enumerate(pairs)]
    for copy in copies:
        copy.start()
    for copy in copies[:4]:
        copy.wait()
    normed = []
    for slab in range(rows // split):
        ks = slice(slab * split, (slab + 1) * split)
        values = x_ref[ks].reshape(split * columns, channels)
        normed.append(kernel_norm(values, gain_ref[...], shift_ref[...]))
        normed_ref[ks] = normed[-1].reshape(split, columns, channels)
    for slab, values in enumerate(normed):
        projected = jnp.dot(values, w_ref[...], preferred_element_type=jnp.float32)
        for i_tile in range(columns // ROWS):
            tiles = []
            for k in range(split):
                first = k * columns + i_tile * ROWS
                part = projected[first : first + ROWS]
                parts = [part[:, n * channels : (n + 1) * channels] for n in range(4)]
                left = jax.nn.sigmoid(parts[0]) * parts[1]
                right = jax.nn.sigmoid(parts[2]) * parts[3]
                both = jnp.concatenate([left, right], axis=0).astype(out_ref.dtype)
                tiles.append(turn(both, k))
            for s, tile in enumerate(spread(tiles)):
                at = slice(i_tile * ROWS, (i_tile + 1) * ROWS)
                lanes = slice(slab * LANES, (slab + 1) * LANES)
                depth_count, _, col_count, row_count = out_ref.shape[:4]
                depth, col, row = s % depth_count, s // depth_count % col_count, s // depth_count // col_count
                out_ref[depth, 1 - core, col, row, at, lanes] = tile[:ROWS]
                out_ref[depth, core, col, row, at, lanes] = tile[ROWS:]
    for copy in copies[4:]:
        copy.wait()


def place_in(*axes):
    place = lax.axis_index(axes[0])
    for axis in axes[1:]:
        place = place * lax.axis_size(axis) + lax.axis_index(axis)
    return place


def lane_place(shape, place):
    return (lax.broadcasted_iota(jnp.int32, shape, 1) - place) & (LANES - 1)


def k_tiles(ref, at):
    return [
        ref[r, at, t * LANES : (t + 1) * LANES]
        for r in range(ref.shape[0])
        for t in range(ref.shape[2] // LANES)
    ]


def fold(tiles, place):
    low = lane_place(tiles[0].shape, place) < LANES // 2
    halves = ([], [])
    for first, second in zip(tiles[::2], tiles[1::2]):
        halves[0].append(jnp.where(low, first, turn(second, LANES // 2)))
        halves[1].append(jnp.where(low, turn(first, LANES // 2), second))
    return [jnp.concatenate(half, axis=1) for half in halves]


def slab_products(split, place, rights, units):
    groups = LANES // split // 2
    shift = split.bit_length() - 1
    position = lane_place((split, LANES), place)
    group = lax.shift_right_logical(position, jnp.int32(shift)) & (groups - 1)
    count = rights[0].shape[1] // LANES
    masks = [
        jnp.concatenate([(group == g).astype(jnp.bfloat16)] * count, axis=1) for g in range(groups)
    ]
    masked = ([], [])
    for unit in units:
        for half, folded in enumerate(fold(unit, place)):
            masked[half].extend(folded * mask for mask in masks)
    low, high = (
        lax.dot_general(
            right, jnp.concatenate(parts, axis=0), NT, preferred_element_type=jnp.float32
        ).astype(jnp.bfloat16)
        for right, parts in zip(rights, masked)
    )
    first_half = lax.broadcasted_iota(jnp.int32, (rights[0].shape[0], LANES), 1) < LANES // 2
    out = []
    for n in range(0, len(units) * LANES // 2, LANES):
        lows, highs = low[:, n : n + LANES], high[:, n : n + LANES]
        out.append(jnp.where(first_half, lows, turn(highs, LANES // 2)))
        out.append(jnp.where(first_half, turn(lows, LANES // 2), highs))
    return out


def pieces_of(split, columns, row_blocks):
    firsts = list(range(0, row_blocks * columns, ROWS))
    per = split // ROWS
    whole = len(firsts) // per * per
    order = [(core, first) for core in (0, 1) for first in firsts[:whole]]
    order += [(core, first) for core in (0, 1) for first in firsts[whole:]]
    return [order[n : n + per] for n in range(0, len(order), per)]


def column_units(ref, split):
    row_count, rows, _ = ref.shape
    columns = rows // row_count
    whole = columns // split * split
    units = [
        k_tiles(ref, slice(target * columns + first, target * columns + first + split))
        for target in range(row_count)
        for first in range(0, whole, split)
    ]
    for target in range(0, row_count, 2):
        halves = [
            k_tiles(ref, slice((target + n) * columns + whole, (target + n + 1) * columns))
            for n in range(2)
        ]
        units.append([jnp.concatenate(parts, axis=0) for parts in zip(*halves)])
    return units


def own_kernel(split, own_ref, right_ref, normed_ref, wg_ref, out_ref, gate_ref, rights_ref):
    place = place_in(*OWNERS)
    rights = fold(k_tiles(right_ref, slice(None)), place)
    for half in range(2):
        rights_ref[half] = rights[half]
    blocks = slab_products(split, place, rights, column_units(own_ref, split))
    for unit, block in enumerate(blocks):
        out_ref[unit] = block
    rows, columns, channels = normed_ref.shape
    normed = normed_ref[...].reshape(rows * columns, channels)
    gate = jax.nn.sigmoid(jnp.dot(normed, wg_ref[...], preferred_element_type=jnp.float32))
    gate_ref[...] = gate.reshape(rows, columns, channels)


def other_kernel(split, done_ref, other_ref, rights_ref, out_ref):
    row_count, rows, _ = other_ref.shape
    place = place_in(*OWNERS)
    rights = [rights_ref[half] for half in range(2)]
    blocks = slab_products(split, place, rights, column_units(other_ref, split))
    whole = rows // row_count // split
    depth_count, col_count, low_count, _, columns, width = out_ref.shape
    last = width - LANES
    lower = lax.broadcasted_iota(jnp.int32, (rows, LANES), 1) & (split // 2) == 0

    def store(target, lane, block):
        high, low = divmod(target, low_count)
        for cy in range(col_count * depth_count):
            col, depth = divmod(cy, depth_count)
            piece = block[cy * columns : (cy + 1) * columns]
            out_ref[depth, col, low, high, :, lane : lane + LANES] = piece

    for target in range(row_count):
        for slab in range(whole):
            unit = target * whole + slab
            store(target, slab * LANES, done_ref[unit])
            store(target, (whole + slab) * LANES, blocks[unit])
    for pair in range(row_count // 2):
        unit = row_count * whole + pair
        firsts, seconds = done_ref[unit], blocks[unit]
        store(2 * pair, last, jnp.where(lower, firsts, turn(seconds, split // 2)))
        store(2 * pair + 1, last, jnp.where(lower, turn(firsts, -(split // 2)), seconds))


def output_kernel(split, slabs, sums_ref, gate_ref, gain_ref, shift_ref, w_ref, out_ref):
    depth_count, col_count, low_count, _, columns, _ = sums_ref.shape
    channels = out_ref.shape[2]
    parity = 1 - lax.axis_index("core")

    def finish(tiles, n, js):
        normed = kernel_norm(jnp.concatenate(tiles, axis=0), gain_ref[...], shift_ref[...])
        projected = jnp.dot(normed, w_ref[...], preferred_element_type=jnp.float32)
        for piece, (core, first) in enumerate(slabs[n]):
            block, inside = divmod(first, columns)
            core = parity if core == 0 else 1 - parity
            at = pl.ds((2 * block + core) * columns + inside, ROWS)
            value = projected[piece * ROWS * ROWS : (piece + 1) * ROWS * ROWS]
            value = value.reshape(ROWS, ROWS, channels)
            out_ref[at, js, :] = (gate_ref[at, js, :] * value).astype(out_ref.dtype)

    units = [
        (n, slice(first, first + ROWS)) for n in range(len(slabs)) for first in range(0, columns, ROWS)
    ]
    for start in range(0, len(units), 2):
        both = units[start : start + 2]
        tiles = []
        for s in range(split):
            rest, depth = divmod(s, depth_count)
            rest, col = divmod(rest, col_count)
            high, low = divmod(rest, low_count)
            parts = [
                sums_ref[depth, col, low, high, js, n * LANES : (n + 1) * LANES] for n, js in both
            ]
            tiles.append(turn(jnp.concatenate(parts, axis=0), s))
        tiles = [turn(tile, -i) for i, tile in enumerate(spread(tiles))]
        for at, (n, js) in enumerate(both):
            finish([tile[at * ROWS : (at + 1) * ROWS] for tile in tiles], n, js)


VMEM = pl.BlockSpec(memory_space=pltpu.VMEM)
HBM = pl.BlockSpec(memory_space=pltpu.HBM)


def call(kernel, name, out_shape, specs, flops, *arrays, scratch=()):
    outs = jax.tree.leaves(out_shape)
    moved = sum(a.size * a.dtype.itemsize for a in [*arrays, *outs])
    return pl.pallas_call(
        kernel,
        name=name,
        out_shape=out_shape,
        in_specs=specs,
        out_specs=jax.tree.map(lambda _: VMEM, out_shape),
        scratch_shapes=scratch,
        cost_estimate=pl.CostEstimate(flops=flops, bytes_accessed=moved, transcendentals=0),
        compiler_params=pltpu.CompilerParams(vmem_limit_bytes=VMEM_LIMIT),
    )(*arrays)


def fast_device(pair_input, in_gain, in_shift, w_proj, w_gate, out_gain, out_shift, w_out):
    rows, columns, channels = pair_input.shape
    high_count, low_count, col_count, depth_count = (lax.axis_size(axis) for axis in OWNERS)
    row_count = high_count * low_count
    split = row_count * col_count * depth_count
    width = rows // split * LANES
    per_row = split // row_count
    slabs = pieces_of(split, columns, rows // (2 * columns))
    units = row_count * (rows // 2 // split) + row_count // 2
    bf16, f32 = jnp.bfloat16, jnp.float32
    shape = jax.ShapeDtypeStruct
    gains = [a.reshape(1, channels) for a in (in_gain, in_shift, out_gain, out_shift)]
    flops = 4 * rows * columns * channels * channels

    edges, normed, wg, og, os, wo = call(
        functools.partial(edges_kernel, split),
        "edges",
        (
            shape((depth_count, 2, col_count, row_count, columns, width), bf16),
            shape(pair_input.shape, bf16),
            shape(w_gate.shape, bf16),
            shape((1, channels), f32),
            shape((1, channels), f32),
            shape(w_out.shape, bf16),
        ),
        [HBM] * 8,
        2 * flops,
        *(
            pltpu.with_memory_space_constraint(a, pltpu.HBM)
            for a in (pair_input, gains[0], gains[1], w_proj, w_gate, gains[2], gains[3], w_out)
        ),
        scratch=(
            pltpu.VMEM(pair_input.shape, bf16),
            pltpu.VMEM((1, channels), f32),
            pltpu.VMEM((1, channels), f32),
            pltpu.VMEM(w_proj.shape, bf16),
            pltpu.SemaphoreType.DMA((8,)),
        ),
    )
    exchange = functools.partial(lax.all_to_all, split_axis=0, concat_axis=0, tiled=True)
    core = lax.axis_index("core").astype(jnp.int32)
    edges, core, partner = lax.optimization_barrier((edges, core, 1 - core))
    grouped = edges.shape
    edges = exchange(
        edges.reshape(2 * split, columns, width), FIRST_ORDER
    ).reshape(grouped)
    def side(array, at):
        piece = lax.dynamic_index_in_dim(array, at, 1, keepdims=False, allow_negative_indices=False)
        return piece.transpose(2, 1, 0, 3, 4).reshape(split, columns, width)

    own, edges = lax.optimization_barrier((side(edges, partner), edges))
    right = side(edges, core)
    other = lax.ppermute(own, "core", [(0, 1), (1, 0)])
    stacked = (row_count, per_row * columns, width)
    own, other, right = (a.reshape(stacked) for a in (own, other, right))
    done, gate, rights = call(
        functools.partial(own_kernel, split),
        "own",
        (
            shape((units, per_row * columns, LANES), bf16),
            shape(pair_input.shape, f32),
            shape((2, per_row * columns, row_count * width // 2), bf16),
        ),
        [VMEM] * 4,
        flops,
        own, right, normed, wg,
    )
    sums = call(
        functools.partial(other_kernel, split),
        "other",
        shape((depth_count, col_count, low_count, high_count, columns, width), bf16),
        [VMEM] * 3,
        flops,
        done, other, rights,
    )
    grouped = sums.shape
    sums = exchange(sums.reshape(split, columns, width), LAST_ORDER).reshape(grouped)
    return call(
        functools.partial(output_kernel, split, slabs),
        "output",
        shape(pair_input.shape, bf16),
        [VMEM] * 5,
        flops // 2,
        sums, gate, og, os, wo,
    )


def suits(mesh, pair_input, w_proj):
    row_count, col_count, depth_count = (mesh.shape[a] for a in ("row", "col", "depth"))
    split = row_count * col_count * depth_count // 2
    rows, columns = pair_input.shape[0] // row_count, pair_input.shape[1] // (col_count * depth_count)
    return (
        depth_count % 2 == 0
        and pair_input.shape[0] == pair_input.shape[1]
        and pair_input.shape[2] == LANES
        and w_proj.shape == (LANES, 4 * LANES)
        and split & (split - 1) == 0
        and split >= 16
        and LANES % (2 * split) == 0
        and row_count % 2 == 0
        and rows % split == 0
        and columns % ROWS == 0
        and rows % (2 * columns) == 0
        and rows // 2 % split == split // 2
    )


def solution(mesh):
    def step(pair_input, in_gain, in_shift, w_proj, w_gate, out_gain, out_shift, w_out):
        if suits(mesh, pair_input, w_proj):
            row_count, col_count, depth_count = mesh.devices.shape
            used = Mesh(
                mesh.devices.reshape(row_count // 2, 2, col_count, depth_count // 2, 2),
                (*OWNERS, "core"),
            )
            pair = P(("row_hi", "row_lo"), ("col", "depth", "core"), None)
            body = fast_device
        else:
            used, pair, body = mesh, P("row", ("col", "depth"), None), plain_device
        return jax.shard_map(
            body,
            mesh=used,
            in_specs=(pair, P(), P(), P(), P(), P(), P(), P()),
            out_specs=pair,
            check_vma=False,
        )(pair_input, in_gain, in_shift, w_proj, w_gate, out_gain, out_shift, w_out)

    return step
```
